32 devices in a mesh: rows: 8 (over y, x, core), dim: 4 (over z).
Axes of the slice: x: 2, y: 2, z: 4, core: 2. Of those that a mesh axis runs over, the one named last changes fastest.
Arguments:
- entity_table: float32 [131072, 512], P(('rows', 'dim')), may hold values from -2.5 to 2.5
- relations: float32 [822, 512], replicated, may hold values from -6 to 6
- thresholds: float32 [64], replicated, may hold values from 0.2 to 2
- head_ids: int32 [2048], replicated, may hold values from 0 to 131071
- rel_ids: int32 [2048], replicated, may hold values from 0 to 821
- thr_idx: int32 [2048], replicated, may hold values from 0 to 63
Outputs:
- serving_table: float32 [131072, 512], P('rows', 'dim')
- fraction: float32 [2048], P(('rows', 'dim'))
The draws below stay inside these ranges and needn't reach their ends.
All inputs are finite; a program needn't handle non-finite values.
Results may differ from the reference program's by a relative error of at most 0.0011.
Values sent between devices are 32-bit elements; how exact they have to be, the bound alone decides.
A program may use at most 128 MiB of HBM per device.

```python
import math
import jax
import jax.numpy as jnp
from jax import lax

D = 512
ENT_DEV = 4096
Q = 2048
NREL = 822
NTHR = 64
ENT = 131072


cluster_count = 32


def draw_entity_table(key, part):
    key_ids = jax.random.fold_in(key, 11)
    key_cent = jax.random.fold_in(key, 12)
    key_vals = jax.random.fold_in(key, 13)
    key_jit = jax.random.fold_in(key, 14)
    member = jax.random.randint(key_ids, (ENT,), 0, cluster_count)
    centers = jnp.clip(jax.random.normal(key_cent, (cluster_count, D), jnp.float32), -6.0, 6.0)
    shared = jnp.take(centers, member, axis=0)
    position = jnp.arange(ENT, dtype=jnp.float32)[:, None] / ENT
    jitter = jax.random.uniform(key_jit, (ENT, 1), jnp.float32, -0.5, 0.5)
    scale = float(D) ** (-0.25) * jnp.exp(math.log(3.0) * (position - 0.5) + jitter)
    noise = jnp.clip(jax.random.normal(key_vals, (ENT, D), jnp.float32), -6.0, 6.0)
    values = scale * (0.8 * shared + 0.6 * noise)
    return jnp.clip(values, -2.5, 2.5).astype(jnp.float32)


def place_ends(drawn, rng, least, top_value):
    spot = [jax.random.randint(jax.random.fold_in(rng, axis), (), 0, length) for axis, length in enumerate(drawn.shape)]
    widest = drawn.shape.index(max(drawn.shape))
    beside = spot[:widest] + [(spot[widest] + 1) % drawn.shape[widest]] + spot[widest + 1:]
    return drawn.at[tuple(spot)].set(least).at[tuple(beside)].set(top_value)


def scatter_about(stream_key, extent, deviation, reach, held_as=jnp.bfloat16):
    result = deviation * jax.random.normal(stream_key, extent, jnp.float32)
    return jnp.clip(result, min=-reach, max=reach).astype(held_as)


def setup_inputs(seed: int = 0) -> dict:
    key_of = jax.random.split(jax.random.key(seed), 7)
    return {
        "entity_table": draw_entity_table(jax.random.fold_in(key_of[6], 71), 0),
        "relations": scatter_about(key_of[1], (NREL, D), 1.0, 6.0, jnp.float32),
        "thresholds": jnp.clip(jax.random.uniform(key_of[2], (NTHR,), jnp.float32, 0.2, 2.0), 0.2, 2.0),
        "head_ids": place_ends(jax.random.randint(key_of[3], (Q,), 0, ENT), jax.random.fold_in(key_of[3], 1), 0, ENT - 1).astype(jnp.int32),
        "rel_ids": place_ends(jax.random.randint(key_of[4], (Q,), 0, NREL), jax.random.fold_in(key_of[4], 1), 0, NREL - 1).astype(jnp.int32),
        "thr_idx": place_ends(jax.random.randint(key_of[5], (Q,), 0, NTHR), jax.random.fold_in(key_of[5], 1), 0, NTHR - 1).astype(jnp.int32),
    }


sharpness = 2.0


def reference(entity_table, relations, thresholds, head_ids, rel_ids, thr_idx):
    head_vecs = jnp.take(entity_table, head_ids, axis=0)
    query = (head_vecs * jnp.take(relations, rel_ids, axis=0)).astype(jnp.bfloat16)
    query = lax.optimization_barrier(query).astype(jnp.float32)
    level = jnp.take(thresholds, thr_idx)
    block = ENT_DEV * 4
    count = ENT // block
    blocks = entity_table.reshape(count, block, D)

    def step(total, rows_block):
        ent_low = lax.optimization_barrier(rows_block.astype(jnp.bfloat16)).astype(jnp.float32)
        score = jnp.dot(query, ent_low.T, precision=lax.Precision.HIGHEST, preferred_element_type=jnp.float32)
        soft = jax.nn.sigmoid(sharpness * (score - level[:, None]))
        return total + jnp.sum(soft, axis=1), None

    total, unused = lax.scan(step, jnp.zeros((Q,), jnp.float32), blocks)
    return entity_table, total * (1.0 / ENT)
```

```python
import functools
import jax
import jax.numpy as jnp
from jax import lax
from jax.sharding import PartitionSpec as P
from jax.experimental import pallas as pl
from jax.experimental.pallas import tpu as pltpu

MESH = pl.DeviceIdType.MESH
sharpness = 2.0
lanes = 128
units = 16
entry = 4


def bits_of(size):
    assert size & (size - 1) == 0
    return size.bit_length() - 1


def kernel(
    R, N, total_ents, head_ids_, rel_ids_, thr_, thr_idx_, rel_, table, *others
):
    slabs = others[:-38]
    (
        serving, frac_out,
        head_ids, rel_ids, thr, thr_idx, rel, arg_sem,
        tab, low, part, recv, full, zsum, zin, zout, qb, lev, frac, fr_rows, fr_dim, fr_sum, fr_all,
        load_sem, own_sem, a2a_send, a2a_recv, ex_send, ex_recv, z_send, z_recv,
        pair_send, pair_recv, f_send, f_recv, g_send, g_recv, last_sem,
    ) = others[-38:]
    r = lax.axis_index("rows")
    d = lax.axis_index("dim")
    core = lax.rem(r, 2)
    n, width = table.shape
    slab = width // N
    Q = part.shape[0]
    half_q = Q // 2
    nrow = bits_of(R)
    ndim = bits_of(N)

    def slab_rows(t, start, rows):
        if slabs:
            return slabs[0].at[t, pl.ds(start, rows), :]
        return table.at[pl.ds(start, rows), pl.ds(pl.multiple_of(t * slab, slab), slab)]

    load = pltpu.make_async_copy(table, tab, load_sem)
    load.start()
    own = pltpu.make_async_copy(
        slab_rows(d, 0, n),
        serving.at[pl.ds(pl.multiple_of(d * n, 8), n), :],
        own_sem,
    )
    own.start()
    pairs = [(head_ids_, head_ids), (rel_ids_, rel_ids), (thr_, thr), (thr_idx_, thr_idx), (rel_, rel)]
    args = [pltpu.make_async_copy(src, dst, arg_sem.at[i]) for i, (src, dst) in enumerate(pairs)]
    for copy in args:
        copy.start()

    row_peers = [lax.rem(r + k, R) for k in range(1, R)]
    dim_peers = [lax.rem(d + k, N) for k in range(1, N)]
    barrier = pltpu.get_barrier_semaphore()
    for t in row_peers:
        pl.semaphore_signal(barrier, inc=1, device_id=(t, d), device_id_type=MESH)
    for t in dim_peers:
        pl.semaphore_signal(barrier, inc=1, device_id=(r, t), device_id_type=MESH)
    pl.semaphore_wait(barrier, R + N - 2)

    first_rows = n * entry // units

    def slab_copies(piece):
        start, rows = ((0, first_rows), (first_rows, n - first_rows))[piece]
        return [
            pltpu.make_async_remote_copy(
                src_ref=slab_rows(t, start, rows),
                dst_ref=serving.at[pl.ds(pl.multiple_of(d * n + start, 8), rows), :],
                send_sem=a2a_send.at[piece, k],
                recv_sem=a2a_recv.at[piece, k],
                device_id=(r, t),
                device_id_type=MESH,
            )
            for k, t in enumerate(dim_peers)
        ]

    a2a = [slab_copies(0), slab_copies(1)]
    for copy in a2a[0]:
        copy.start()

    @pl.when(core == 0)
    def _():
        for copy in a2a[1]:
            copy.start()

    for copy in args:
        copy.wait()
    load.wait()
    first = (r * N + d) * n

    def pick(i, carry):
        base = pl.multiple_of(i * 8, 8)
        rows = []
        for j in range(8):
            local = head_ids[base + j] - first
            owned = jnp.logical_and(local >= 0, local < n)
            row = tab[pl.ds(jnp.clip(local, 0, n - 1), 1), :]
            rows.append(jnp.where(owned, row, jnp.zeros_like(row)))
        part[pl.ds(base, 8), :] = jnp.concatenate(rows, axis=0)
        return carry

    lax.fori_loop(0, Q // 8, pick, 0)

    def bit_and_other(me, b):
        bit = lax.rem(me // (2 ** b), 2)
        return bit, me + (1 - 2 * bit) * (2 ** b)

    def remote(src, dst, sems, at, peer):
        return pltpu.make_async_remote_copy(
            src_ref=src, dst_ref=dst, send_sem=sems[0].at[at], recv_sem=sems[1].at[at],
            device_id=peer, device_id_type=MESH,
        )

    def add_rows(h, dst, dst_at, src, src_at, extra, extra_at):
        rows = min(64, h)

        def add(i, carry):
            step = i * rows
            dst[pl.ds(pl.multiple_of(dst_at + step, 8), rows), :] = (
                src[pl.ds(pl.multiple_of(src_at + step, 8), rows), :]
                + extra[pl.ds(pl.multiple_of(extra_at + step, 8), rows), :]
            )
            return carry

        lax.fori_loop(0, h // rows, add, 0)

    row_bits = list(range(nrow))
    orders = [row_bits, row_bits[:1] + row_bits[:0:-1]]
    ex = (ex_send, ex_recv)

    offset = [0, half_q]
    size = half_q
    into = 0
    for k in range(nrow):
        h = size // 2
        copies = []
        for s in range(2):
            bit, other = bit_and_other(r, orders[s][k])
            gone = pl.multiple_of(offset[s] + (1 - bit) * h, 8)
            copy = remote(
                part.at[pl.ds(gone, h), :],
                recv.at[pl.ds(s * half_q + into, h), :],
                ex, (s, k), (other, d),
            )
            copy.start()
            copies.append(copy)
            offset[s] = pl.multiple_of(offset[s] + bit * h, 8)
        if k == 0:
            def narrow(i, carry):
                at = pl.multiple_of(i * 128, 128)
                low[pl.ds(at, 128), :] = tab[pl.ds(at, 128), :].astype(jnp.bfloat16)
                return carry

            lax.fori_loop(0, n // 128, narrow, 0)
        if k == 1:
            idx = thr_idx[...]

            def choose(t, acc):
                return jnp.where(idx == t, thr[t], acc)

            lev[...] = lax.fori_loop(0, thr.shape[0], choose, jnp.zeros(idx.shape, jnp.float32))
        for s in range(2):
            copies[s].wait()
            if k < nrow - 1:
                add_rows(h, part, offset[s], part, offset[s], recv, s * half_q + into)
            else:
                add_rows(h, zsum, (2 * s + core) * h, part, offset[s], recv, s * half_q + into)
        into += h
        size = h

    partner = (r + 1 - 2 * core, d)
    skip = half_q // 2
    core0_at = [pl.multiple_of(offset[s] - core * skip, 8) for s in range(2)]
    pair = (pair_send, pair_recv)
    there_ = [
        remote(zsum.at[pl.ds(2 * s * size, size), :], zsum.at[pl.ds(2 * s * size, size), :], pair, (0, s), partner)
        for s in range(2)
    ]
    back = [
        remote(zout.at[pl.ds(2 * s * size, size), :], full.at[pl.ds(core0_at[s], size), :], pair, (1, s), partner)
        for s in range(2)
    ]
    zx = (z_send, z_recv)

    @pl.when(core == 0)
    def _():
        for copy in there_:
            copy.start()
        for copy in there_:
            copy.wait_send()
        for copy in back:
            copy.wait_recv()

    @pl.when(core == 1)
    def _():
        for copy in there_:
            copy.wait_recv()
        at, count_, into = 0, 4 * size, 0
        for b in range(ndim):
            h = count_ // 2
            bit, other = bit_and_other(d, b)
            gone = pl.multiple_of(at + (1 - bit) * h, 8)
            copy = remote(zsum.at[pl.ds(gone, h), :], zin.at[pl.ds(into, h), :], zx, b, (r, other))
            copy.start()
            at = pl.multiple_of(at + bit * h, 8)
            copy.wait()
            add_rows(h, zsum, at, zsum, at, zin, into)
            into += h
            count_ = h

        def form(i, carry):
            z = pl.multiple_of(at + i * 8, 8)
            slot = z // size
            s = slot // 2
            c = slot - 2 * s
            q = (1 - s) * core0_at[0] + s * core0_at[1] + c * skip + (z - slot * size)
            rows = [rel[pl.ds(rel_ids[q + j], 1), :] for j in range(8)]
            zout[pl.ds(z, 8), :] = zsum[pl.ds(z, 8), :] * jnp.concatenate(rows, axis=0)
            return carry

        lax.fori_loop(0, count_ // 8, form, 0)
        for b in reversed(range(ndim)):
            bit, other = bit_and_other(d, b)
            here = zout.at[pl.ds(at, count_), :]
            copy = remote(here, here, zx, ndim + b, (r, other))
            copy.start()
            if b == 0:
                for late in a2a[1]:
                    late.start()
            copy.wait()
            at = pl.multiple_of(at - bit * count_, 8)
            count_ = 2 * count_
        for copy in back:
            copy.start()
        for s in range(2):
            rows = min(64, size)

            def take(i, carry, s=s):
                step = i * rows
                full[pl.ds(pl.multiple_of(offset[s] + step, 8), rows), :] = (
                    zout[pl.ds(pl.multiple_of((2 * s + 1) * size + step, 8), rows), :]
                )
                return carry

            lax.fori_loop(0, size // rows, take, 0)
        for copy in back:
            copy.wait_send()

    def count_pair(q0, q1):
        qb[:lanes, :] = full[pl.ds(q0, lanes), :].astype(jnp.bfloat16)
        qb[lanes:, :] = full[pl.ds(q1, lanes), :].astype(jnp.bfloat16)
        i0 = q0 // lanes
        i1 = q1 // lanes
        level = jnp.concatenate([lev[i0], lev[i1]], axis=1)
        rows = 512

        def tile(i, acc):
            at = pl.multiple_of(i * rows, rows)
            score = lax.dot_general(
                low[pl.ds(at, rows), :], qb[...], (((1,), (1,)), ((), ())),
                preferred_element_type=jnp.float32,
            )
            soft = jax.nn.sigmoid(sharpness * (score - level))
            return acc + jnp.sum(soft.reshape(rows // 8, 8, 2 * lanes), axis=0)

        acc = lax.fori_loop(0, n // rows, tile, jnp.zeros((8, 2 * lanes), jnp.float32))
        share = jnp.sum(acc, axis=0, keepdims=True) * (1.0 / total_ents)
        frac[i0] = share[:, :lanes]
        frac[i1] = share[:, lanes:]

    def count(starts_, rows):
        def body(i, carry):
            count_pair(pl.multiple_of(starts_[0] + i * lanes, lanes), pl.multiple_of(starts_[1] + i * lanes, lanes))
            return carry

        lax.fori_loop(0, rows // lanes, body, 0)

    pending = None
    counted = False
    if size >= lanes:
        pending = (list(offset), size)
        counted = True
    for k in reversed(range(nrow)):
        copies = []
        there = []
        for s in range(2):
            bit, other = bit_and_other(r, orders[s][k])
            here = full.at[pl.ds(offset[s], size), :]
            copy = remote(here, here, ex, (s, nrow + k), (other, d))
            copy.start()
            copies.append(copy)
            there.append(pl.multiple_of(offset[s] + (1 - 2 * bit) * size, 8))
            offset[s] = pl.multiple_of(offset[s] - bit * size, 8)
        if pending is not None:
            count(*pending)
            pending = None
        for copy in copies:
            copy.wait()
        size = 2 * size
        if size >= lanes:
            pending = (there, size // 2) if counted else (list(offset), size)
            counted = True
    count(*pending)

    per = frac.shape[0] // R
    chips = R // 2

    def row_share(k):
        t = 2 * lax.rem(r // 2 + k, chips)
        slot = R - 2 * k - 1 + core if k else 0
        return pltpu.make_async_remote_copy(
            src_ref=frac.at[pl.ds(t * per, 2 * per)], dst_ref=fr_rows.at[slot],
            send_sem=f_send.at[k], recv_sem=f_recv.at[slot],
            device_id=(t, d), device_id_type=MESH,
        )

    shares = [row_share(k) for k in range(chips)]
    last = pltpu.make_async_remote_copy(
        src_ref=fr_all, dst_ref=fr_all, send_sem=last_sem.at[0], recv_sem=last_sem.at[1],
        device_id=partner, device_id_type=MESH,
    )
    for copy in shares[1:]:
        copy.start()

    @pl.when(core == 1)
    def _():
        shares[0].start()
        shares[0].wait_send()

    for copy in shares[1:]:
        copy.wait_send()

    @pl.when(core == 0)
    def _():
        total = frac[pl.ds(r * per, 2 * per)]
        for k in range(R - 1):
            pltpu.make_async_remote_copy(
                src_ref=frac.at[pl.ds(r * per, 2 * per)], dst_ref=fr_rows.at[k],
                send_sem=f_send.at[0], recv_sem=f_recv.at[k],
                device_id=(row_peers[k], d), device_id_type=MESH,
            ).wait_recv()
            total = total + fr_rows[k]
        fr_sum[...] = total
        sends = []
        for k, t in enumerate(dim_peers):
            copy = pltpu.make_async_remote_copy(
                src_ref=fr_sum, dst_ref=fr_dim.at[N - 2 - k],
                send_sem=g_send.at[k], recv_sem=g_recv.at[N - 2 - k],
                device_id=(r, t), device_id_type=MESH,
            )
            copy.start()
            sends.append(copy)
        for k in range(N - 1):
            sends[k].wait_send()
            pltpu.make_async_remote_copy(
                src_ref=fr_sum, dst_ref=fr_dim.at[k],
                send_sem=g_send.at[k], recv_sem=g_recv.at[k],
                device_id=(r, dim_peers[k]), device_id_type=MESH,
            ).wait_recv()
            total = total + fr_dim[k]
        fr_all[...] = total
        last.start()
        last.wait_send()

    @pl.when(core == 1)
    def _():
        last.wait_recv()

    mine = frac_out.shape[1]
    row = fr_all[core * per + d * mine // lanes]
    place = lax.rem(d * mine, lanes) // mine
    out = row[:, :mine]
    for j in range(1, lanes // mine):
        out = jnp.where(place == j, row[:, j * mine:(j + 1) * mine], out)
    frac_out[...] = out
    own.wait()
    for copies in a2a:
        for copy in copies:
            copy.wait()


def shards(entity_table, relations, thresholds, head_ids, rel_ids, thr_idx):
    R = lax.axis_size("rows")
    N = lax.axis_size("dim")
    n, width = entity_table.shape
    Q = head_ids.shape[0]
    blocks = Q // lanes
    per = blocks // R
    group = 2 * Q // R
    f32 = jnp.float32
    DMA = pltpu.SemaphoreType.DMA
    vmem = pl.BlockSpec(memory_space=pltpu.VMEM)
    hbm = pl.BlockSpec(memory_space=pltpu.HBM)
    anywhere = pl.BlockSpec(memory_space=pl.ANY)
    mine = Q // (R * N)
    operands = [head_ids, rel_ids, thresholds, thr_idx.reshape(blocks, 1, lanes), relations, entity_table]
    if (width // N) % lanes:
        operands.append(entity_table.reshape(n, N, width // N).transpose(1, 0, 2))
    serving, share = pl.pallas_call(
        functools.partial(kernel, R, N, n * R * N),
        out_shape=(
            pltpu.VMEM((n * N, width // N), f32),
            jax.ShapeDtypeStruct((1, mine), f32),
        ),
        in_specs=[hbm] * len(operands),
        out_specs=(anywhere, vmem),
        scratch_shapes=[
            pltpu.SMEM((Q,), jnp.int32),
            pltpu.SMEM((Q,), jnp.int32),
            pltpu.SMEM(thresholds.shape, f32),
            pltpu.VMEM((blocks, 1, lanes), jnp.int32),
            pltpu.VMEM(relations.shape, f32),
            DMA((5,)),
            pltpu.VMEM((n, width), f32),
            pltpu.VMEM((n, width), jnp.bfloat16),
            pltpu.VMEM((Q, width), f32),
            pltpu.VMEM((Q, width), f32),
            pltpu.VMEM((Q, width), f32),
            pltpu.VMEM((group, width), f32),
            pltpu.VMEM((group, width), f32),
            pltpu.VMEM((group, width), f32),
            pltpu.VMEM((2 * lanes, width), jnp.bfloat16),
            pltpu.VMEM((blocks, 1, lanes), f32),
            pltpu.VMEM((blocks, 1, lanes), f32),
            pltpu.VMEM((R - 1, 2 * per, 1, lanes), f32),
            pltpu.VMEM((N - 1, 2 * per, 1, lanes), f32),
            pltpu.VMEM((2 * per, 1, lanes), f32),
            pltpu.VMEM((2 * per, 1, lanes), f32),
            DMA, DMA,
            DMA((2, N - 1)), DMA((2, N - 1)),
            DMA((2, 2 * bits_of(R))), DMA((2, 2 * bits_of(R))),
            DMA((2 * bits_of(N),)), DMA((2 * bits_of(N),)),
            DMA((2, 2)), DMA((2, 2)),
            DMA((R // 2,)), DMA((R - 1,)),
            DMA((N - 1,)), DMA((N - 1,)),
            DMA((2,)),
        ],
        compiler_params=pltpu.CompilerParams(
            collective_id=0, has_side_effects=True, vmem_limit_bytes=40 * 2**20
        ),
    )(*[pltpu.with_memory_space_constraint(x, pltpu.HBM) for x in operands])
    return serving, share.reshape(mine)


def solution(mesh):
    placed = (P(("rows", "dim"), None), P(), P(), P(), P(), P())
    return jax.shard_map(
        shards,
        mesh=mesh,
        in_specs=placed,
        out_specs=(P("rows", "dim"), P(("rows", "dim"))),
        check_vma=False,
    )
```

```python
import functools
import jax
import jax.numpy as jnp
from jax import lax
from jax.sharding import PartitionSpec as P
from jax.experimental import pallas as pl
from jax.experimental.pallas import tpu as pltpu

MESH = pl.DeviceIdType.MESH
sharpness = 2.0
lanes = 128
units = 16
entry = 4


def bits_of(size):
    assert size & (size - 1) == 0
    return size.bit_length() - 1


def kernel(
    R, N, total_ents, head_ids_, rel_ids_, thr_, thr_idx_, rel_, table, *others
):
    slabs = others[:-40]
    (
        serving, frac_out,
        head_ids, rel_ids, thr, thr_idx, rel, arg_sem,
        tab, low, part, recv, full, zsum, zin, zout, qb, lev, frac, fr_pair, fr_in, fr_dim, fr_sum, fr_all,
        load_sem, own_sem, a2a_send, a2a_recv, ex_send, ex_recv, z_send, z_recv,
        pair_send, pair_recv, f_send, f_recv, g_send, g_recv, last_send, last_recv,
    ) = others[-40:]
    r = lax.axis_index("rows")
    d = lax.axis_index("dim")
    core = lax.rem(r, 2)
    n, width = table.shape
    slab = width // N
    Q = part.shape[0]
    half_q = Q // 2
    nrow = bits_of(R)
    ndim = bits_of(N)

    def slab_rows(t, start, rows):
        if slabs:
            return slabs[0].at[t, pl.ds(start, rows), :]
        return table.at[pl.ds(start, rows), pl.ds(pl.multiple_of(t * slab, slab), slab)]

    def bit_and_other(me, b):
        bit = lax.rem(me // (2 ** b), 2)
        return bit, me + (1 - 2 * bit) * (2 ** b)

    row_peers = [bit_and_other(r, b)[1] for b in range(nrow)]
    dim_peers = []
    for k in range(1, N):
        t = d
        for b in range(ndim):
            if k // 2 ** b % 2:
                t = t + (bit_and_other(d, b)[1] - d)
        dim_peers.append(t)
    barrier = pltpu.get_barrier_semaphore()
    for t in dim_peers:
        pl.semaphore_signal(barrier, inc=1, device_id=(r, t), device_id_type=MESH)
    for t in row_peers:
        pl.semaphore_signal(barrier, inc=1, device_id=(t, d), device_id_type=MESH)
    load = pltpu.make_async_copy(table, tab, load_sem)
    load.start()
    own = pltpu.make_async_copy(
        slab_rows(d, 0, n),
        serving.at[pl.ds(pl.multiple_of(d * n, 8), n), :],
        own_sem,
    )
    own.start()
    pairs = [(head_ids_, head_ids), (rel_ids_, rel_ids), (thr_, thr), (thr_idx_, thr_idx), (rel_, rel)]
    args = [pltpu.make_async_copy(src, dst, arg_sem.at[i]) for i, (src, dst) in enumerate(pairs)]
    for copy in args:
        copy.start()
    pl.semaphore_wait(barrier, len(row_peers) + len(dim_peers))

    first_rows = n * entry // units

    def slab_copies(piece):
        start, rows = ((0, first_rows), (first_rows, n - first_rows))[piece]
        return [
            pltpu.make_async_remote_copy(
                src_ref=slab_rows(t, start, rows),
                dst_ref=serving.at[pl.ds(pl.multiple_of(d * n + start, 8), rows), :],
                send_sem=a2a_send.at[piece, k],
                recv_sem=a2a_recv.at[piece, k],
                device_id=(r, t),
                device_id_type=MESH,
            )
            for k, t in enumerate(dim_peers)
        ]

    a2a = [slab_copies(0), slab_copies(1)]
    for copy in a2a[0]:
        copy.start()

    @pl.when(core == 0)
    def _():
        for copy in a2a[1]:
            copy.start()

    for copy in args:
        copy.wait()
    load.wait()
    first = (r * N + d) * n

    def pick(i, carry):
        base = pl.multiple_of(i * 8, 8)
        rows = []
        for j in range(8):
            local = head_ids[base + j] - first
            owned = jnp.logical_and(local >= 0, local < n)
            row = tab[pl.ds(jnp.clip(local, 0, n - 1), 1), :]
            rows.append(jnp.where(owned, row, jnp.zeros_like(row)))
        part[pl.ds(base, 8), :] = jnp.concatenate(rows, axis=0)
        return carry

    lax.fori_loop(0, Q // 8, pick, 0)

    def remote(src, dst, sems, at, peer):
        return pltpu.make_async_remote_copy(
            src_ref=src, dst_ref=dst, send_sem=sems[0].at[at], recv_sem=sems[1].at[at],
            device_id=peer, device_id_type=MESH,
        )

    def add_rows(h, dst, dst_at, src, src_at, extra, extra_at):
        rows = min(64, h)

        def add(i, carry):
            step = i * rows
            dst[pl.ds(pl.multiple_of(dst_at + step, 8), rows), :] = (
                src[pl.ds(pl.multiple_of(src_at + step, 8), rows), :]
                + extra[pl.ds(pl.multiple_of(extra_at + step, 8), rows), :]
            )
            return carry

        lax.fori_loop(0, h // rows, add, 0)

    row_bits = list(range(nrow))
    orders = [row_bits, row_bits[:1] + row_bits[:0:-1]]
    ex = (ex_send, ex_recv)

    offset = [0, half_q]
    size = half_q
    into = 0
    for k in range(nrow):
        h = size // 2
        copies = []
        for s in range(2):
            bit, other = bit_and_other(r, orders[s][k])
            gone = pl.multiple_of(offset[s] + (1 - bit) * h, 8)
            copy = remote(
                part.at[pl.ds(gone, h), :],
                recv.at[pl.ds(s * half_q + into, h), :],
                ex, (s, k), (other, d),
            )
            copy.start()
            copies.append(copy)
            offset[s] = pl.multiple_of(offset[s] + bit * h, 8)
        if k == 0:
            def narrow(i, carry):
                at = pl.multiple_of(i * 128, 128)
                low[pl.ds(at, 128), :] = tab[pl.ds(at, 128), :].astype(jnp.bfloat16)
                return carry

            lax.fori_loop(0, n // 128, narrow, 0)
        if k == 1:
            idx = thr_idx[...]

            def choose(t, acc):
                return jnp.where(idx == t, thr[t], acc)

            lev[...] = lax.fori_loop(0, thr.shape[0], choose, jnp.zeros(idx.shape, jnp.float32))
        for s in range(2):
            copies[s].wait()
            if k < nrow - 1:
                add_rows(h, part, offset[s], part, offset[s], recv, s * half_q + into)
            else:
                add_rows(h, zsum, (2 * s + core) * h, part, offset[s], recv, s * half_q + into)
        into += h
        size = h

    partner = (r + 1 - 2 * core, d)
    skip = half_q // 2
    core0_at = [pl.multiple_of(offset[s] - core * skip, 8) for s in range(2)]
    pair = (pair_send, pair_recv)
    there_ = [
        remote(zsum.at[pl.ds(2 * s * size, size), :], zsum.at[pl.ds(2 * s * size, size), :], pair, (0, s), partner)
        for s in range(2)
    ]
    back = [
        remote(zout.at[pl.ds(2 * s * size, size), :], full.at[pl.ds(core0_at[s], size), :], pair, (1, s), partner)
        for s in range(2)
    ]
    zx = (z_send, z_recv)

    @pl.when(core == 0)
    def _():
        for copy in there_:
            copy.start()
        for copy in there_:
            copy.wait_send()
        for copy in back:
            copy.wait_recv()

    @pl.when(core == 1)
    def _():
        for copy in there_:
            copy.wait_recv()
        at, count_, into = 0, 4 * size, 0
        for b in range(ndim):
            h = count_ // 2
            bit, other = bit_and_other(d, b)
            gone = pl.multiple_of(at + (1 - bit) * h, 8)
            copy = remote(zsum.at[pl.ds(gone, h), :], zin.at[pl.ds(into, h), :], zx, b, (r, other))
            copy.start()
            at = pl.multiple_of(at + bit * h, 8)
            copy.wait()
            add_rows(h, zsum, at, zsum, at, zin, into)
            into += h
            count_ = h

        def form(i, carry):
            z = pl.multiple_of(at + i * 8, 8)
            slot = z // size
            s = slot // 2
            c = slot - 2 * s
            q = (1 - s) * core0_at[0] + s * core0_at[1] + c * skip + (z - slot * size)
            rows = [rel[pl.ds(rel_ids[q + j], 1), :] for j in range(8)]
            zout[pl.ds(z, 8), :] = zsum[pl.ds(z, 8), :] * jnp.concatenate(rows, axis=0)
            return carry

        lax.fori_loop(0, count_ // 8, form, 0)
        for b in reversed(range(ndim)):
            bit, other = bit_and_other(d, b)
            here = zout.at[pl.ds(at, count_), :]
            copy = remote(here, here, zx, ndim + b, (r, other))
            copy.start()
            if b == 0:
                for late in a2a[1]:
                    late.start()
            copy.wait()
            at = pl.multiple_of(at - bit * count_, 8)
            count_ = 2 * count_
        for copy in back:
            copy.start()
        for s in range(2):
            rows = min(64, size)

            def take(i, carry, s=s):
                step = i * rows
                full[pl.ds(pl.multiple_of(offset[s] + step, 8), rows), :] = (
                    zout[pl.ds(pl.multiple_of((2 * s + 1) * size + step, 8), rows), :]
                )
                return carry

            lax.fori_loop(0, size // rows, take, 0)
        for copy in back:
            copy.wait_send()

    def count_pair(q0, q1):
        qb[:lanes, :] = full[pl.ds(q0, lanes), :].astype(jnp.bfloat16)
        qb[lanes:, :] = full[pl.ds(q1, lanes), :].astype(jnp.bfloat16)
        i0 = q0 // lanes
        i1 = q1 // lanes
        level = jnp.concatenate([lev[i0], lev[i1]], axis=1)
        rows = 512

        def tile(i, acc):
            at = pl.multiple_of(i * rows, rows)
            score = lax.dot_general(
                low[pl.ds(at, rows), :], qb[...], (((1,), (1,)), ((), ())),
                preferred_element_type=jnp.float32,
            )
            soft = jax.nn.sigmoid(sharpness * (score - level))
            return acc + jnp.sum(soft.reshape(rows // 8, 8, 2 * lanes), axis=0)

        acc = lax.fori_loop(0, n // rows, tile, jnp.zeros((8, 2 * lanes), jnp.float32))
        share = jnp.sum(acc, axis=0, keepdims=True) * (1.0 / total_ents)
        frac[i0] = share[:, :lanes]
        frac[i1] = share[:, lanes:]

    def count(starts_, rows):
        def body(i, carry):
            count_pair(pl.multiple_of(starts_[0] + i * lanes, lanes), pl.multiple_of(starts_[1] + i * lanes, lanes))
            return carry

        lax.fori_loop(0, rows // lanes, body, 0)

    pending = None
    counted = False
    if size >= lanes:
        pending = (list(offset), size)
        counted = True
    for k in reversed(range(nrow)):
        copies = []
        there = []
        for s in range(2):
            bit, other = bit_and_other(r, orders[s][k])
            here = full.at[pl.ds(offset[s], size), :]
            copy = remote(here, here, ex, (s, nrow + k), (other, d))
            copy.start()
            copies.append(copy)
            there.append(pl.multiple_of(offset[s] + (1 - 2 * bit) * size, 8))
            offset[s] = pl.multiple_of(offset[s] - bit * size, 8)
        if pending is not None:
            count(*pending)
            pending = None
        for copy in copies:
            copy.wait()
        size = 2 * size
        if size >= lanes:
            pending = (there, size // 2) if counted else (list(offset), size)
            counted = True
    count(*pending)

    per = frac.shape[0] // R
    fx = (f_send, f_recv)
    handed = remote(frac, fr_pair, fx, 0, partner)
    last = remote(fr_all, fr_all, (last_send, last_recv), 0, partner)

    @pl.when(core == 1)
    def _():
        handed.start()
        handed.wait_send()
        last.wait_recv()

    @pl.when(core == 0)
    def _():
        handed.wait_recv()
        frac[...] = frac[...] + fr_pair[...]
        at, held, into = 0, frac.shape[0], 0
        for b in reversed(range(1, nrow)):
            h = held // 2
            bit, other = bit_and_other(r, b)
            copy = remote(frac.at[pl.ds(at + (1 - bit) * h, h)], fr_in.at[pl.ds(into, h)], fx, b, (other, d))
            copy.start()
            at = at + bit * h
            copy.wait()
            frac[pl.ds(at, h)] = frac[pl.ds(at, h)] + fr_in[pl.ds(into, h)]
            into += h
            held = h
        total = frac[pl.ds(at, held)]
        fr_sum[...] = total
        sends = []
        for k, t in enumerate(dim_peers):
            copy = pltpu.make_async_remote_copy(
                src_ref=fr_sum, dst_ref=fr_dim.at[k],
                send_sem=g_send.at[k], recv_sem=g_recv.at[k],
                device_id=(r, t), device_id_type=MESH,
            )
            copy.start()
            sends.append(copy)
        for k in range(N - 1):
            sends[k].wait()
            total = total + fr_dim[k]
        fr_all[...] = total
        last.start()
        last.wait_send()

    mine = frac_out.shape[1]
    row = fr_all[core * per + d * mine // lanes]
    place = lax.rem(d * mine, lanes) // mine
    out = row[:, :mine]
    for j in range(1, lanes // mine):
        out = jnp.where(place == j, row[:, j * mine:(j + 1) * mine], out)
    frac_out[...] = out
    own.wait()
    for copies in a2a:
        for copy in copies:
            copy.wait()


def shards(entity_table, relations, thresholds, head_ids, rel_ids, thr_idx):
    R = lax.axis_size("rows")
    N = lax.axis_size("dim")
    n, width = entity_table.shape
    Q = head_ids.shape[0]
    blocks = Q // lanes
    per = blocks // R
    group = 2 * Q // R
    f32 = jnp.float32
    DMA = pltpu.SemaphoreType.DMA
    vmem = pl.BlockSpec(memory_space=pltpu.VMEM)
    hbm = pl.BlockSpec(memory_space=pltpu.HBM)
    anywhere = pl.BlockSpec(memory_space=pl.ANY)
    mine = Q // (R * N)
    operands = [head_ids, rel_ids, thresholds, thr_idx.reshape(blocks, 1, lanes), relations, entity_table]
    if (width // N) % lanes:
        operands.append(entity_table.reshape(n, N, width // N).transpose(1, 0, 2))
    serving, share = pl.pallas_call(
        functools.partial(kernel, R, N, n * R * N),
        out_shape=(
            pltpu.VMEM((n * N, width // N), f32),
            jax.ShapeDtypeStruct((1, mine), f32),
        ),
        in_specs=[hbm] * len(operands),
        out_specs=(anywhere, vmem),
        scratch_shapes=[
            pltpu.SMEM((Q,), jnp.int32),
            pltpu.SMEM((Q,), jnp.int32),
            pltpu.SMEM(thresholds.shape, f32),
            pltpu.VMEM((blocks, 1, lanes), jnp.int32),
            pltpu.VMEM(relations.shape, f32),
            DMA((5,)),
            pltpu.VMEM((n, width), f32),
            pltpu.VMEM((n, width), jnp.bfloat16),
            pltpu.VMEM((Q, width), f32),
            pltpu.VMEM((Q, width), f32),
            pltpu.VMEM((Q, width), f32),
            pltpu.VMEM((group, width), f32),
            pltpu.VMEM((group, width), f32),
            pltpu.VMEM((group, width), f32),
            pltpu.VMEM((2 * lanes, width), jnp.bfloat16),
            pltpu.VMEM((blocks, 1, lanes), f32),
            pltpu.VMEM((blocks, 1, lanes), f32),
            pltpu.VMEM((blocks, 1, lanes), f32),
            pltpu.VMEM((blocks, 1, lanes), f32),
            pltpu.VMEM((N - 1, 2 * per, 1, lanes), f32),
            pltpu.VMEM((2 * per, 1, lanes), f32),
            pltpu.VMEM((2 * per, 1, lanes), f32),
            DMA, DMA,
            DMA((2, N - 1)), DMA((2, N - 1)),
            DMA((2, 2 * bits_of(R))), DMA((2, 2 * bits_of(R))),
            DMA((2 * bits_of(N),)), DMA((2 * bits_of(N),)),
            DMA((2, 2)), DMA((2, 2)),
            DMA((bits_of(R),)), DMA((bits_of(R),)),
            DMA((N - 1,)), DMA((N - 1,)),
            DMA((1,)), DMA((1,)),
        ],
        compiler_params=pltpu.CompilerParams(
            collective_id=0, has_side_effects=True, vmem_limit_bytes=40 * 2**20
        ),
    )(*[pltpu.with_memory_space_constraint(x, pltpu.HBM) for x in operands])
    return serving, share.reshape(mine)


def solution(mesh):
    placed = (P(("rows", "dim"), None), P(), P(), P(), P(), P())
    return jax.shard_map(
        shards,
        mesh=mesh,
        in_specs=placed,
        out_specs=(P("rows", "dim"), P(("rows", "dim"))),
        check_vma=False,
    )
```

```python
import functools
import jax
import jax.numpy as jnp
from jax import lax
from jax.sharding import PartitionSpec as P
from jax.experimental import pallas as pl
from jax.experimental.pallas import tpu as pltpu

MESH = pl.DeviceIdType.MESH
sharpness = 2.0
lanes = 128
units = 16
entry = 3


def bits_of(size):
    assert size & (size - 1) == 0
    return size.bit_length() - 1


def kernel(
    R, N, total_ents, head_ids_, rel_ids_, thr_, thr_idx_, rel_, table, *others
):
    slabs = others[:-41]
    (
        serving, frac_out,
        head_ids, rel_ids, thr, thr_idx, rel, arg_sem,
        tab, low, part, recv, full, zsum, zin, zout, qb, lev, frac, fr_pair, fr_in, fr_dim, fr_sum, fr_all,
        load_sem, own_sem, a2a_send, a2a_recv, ex_send, ex_recv, z_send, z_recv,
        pair_send, pair_recv, f_send, f_recv, g_send, g_recv, last_send, last_recv, answer,
    ) = others[-41:]
    r = lax.axis_index("rows")
    d = lax.axis_index("dim")
    core = lax.rem(r, 2)
    n, width = table.shape
    slab = width // N
    Q = part.shape[0]
    half_q = Q // 2
    nrow = bits_of(R)
    ndim = bits_of(N)

    def slab_rows(t, start, rows):
        if slabs:
            return slabs[0].at[t, pl.ds(start, rows), :]
        return table.at[pl.ds(start, rows), pl.ds(pl.multiple_of(t * slab, slab), slab)]

    def bit_and_other(me, b):
        bit = lax.rem(me // (2 ** b), 2)
        return bit, me + (1 - 2 * bit) * (2 ** b)

    dim_peers = []
    for k in range(1, N):
        t = d
        for b in range(ndim):
            if k // 2 ** b % 2:
                t = t + (bit_and_other(d, b)[1] - d)
        dim_peers.append(t)
    def ahead(j):
        return (r, lax.rem(d + j, N)), d + j < N

    def behind(j):
        return (r, lax.rem(d + N - j, N)), d >= j

    row_pairs = [bit_and_other(r, b) for b in range(nrow)]
    barrier = pltpu.get_barrier_semaphore()
    leaders = d
    for j in range(1, N):
        peer, leads = ahead(j)

        @pl.when(leads)
        def _(peer=peer):
            pl.semaphore_signal(barrier, inc=1, device_id=peer, device_id_type=MESH)

    for bit, other in row_pairs:
        leaders = leaders + bit

        @pl.when(bit == 0)
        def _(other=other):
            pl.semaphore_signal(barrier, inc=1, device_id=(other, d), device_id_type=MESH)

    load = pltpu.make_async_copy(table, tab, load_sem)
    load.start()
    own = pltpu.make_async_copy(
        slab_rows(d, 0, n),
        serving.at[pl.ds(pl.multiple_of(d * n, 8), n), :],
        own_sem,
    )
    own.start()
    pairs = [(head_ids_, head_ids), (rel_ids_, rel_ids), (thr_, thr), (thr_idx_, thr_idx), (rel_, rel)]
    args = [pltpu.make_async_copy(src, dst, arg_sem.at[i]) for i, (src, dst) in enumerate(pairs)]
    for copy in args:
        copy.start()

    @pl.when(leaders > 0)
    def _():
        pl.semaphore_wait(barrier, leaders)

    for j in range(1, N):
        peer, follows = behind(j)

        @pl.when(follows)
        def _(j=j, peer=peer):
            pl.semaphore_signal(answer.at[j - 1], inc=1, device_id=peer, device_id_type=MESH)

    for b, (bit, other) in enumerate(row_pairs):
        @pl.when(bit == 1)
        def _(b=b, other=other):
            pl.semaphore_signal(answer.at[N - 1 + b], inc=1, device_id=(other, d), device_id_type=MESH)

    first_rows = n * entry // units

    def slab_copies(piece):
        start, rows = ((0, first_rows), (first_rows, n - first_rows))[piece]
        return [
            pltpu.make_async_remote_copy(
                src_ref=slab_rows(t, start, rows),
                dst_ref=serving.at[pl.ds(pl.multiple_of(d * n + start, 8), rows), :],
                send_sem=a2a_send.at[piece, k],
                recv_sem=a2a_recv.at[piece, k],
                device_id=(r, t),
                device_id_type=MESH,
            )
            for k, t in enumerate(dim_peers if piece else [lax.rem(d + j, N) for j in range(1, N)])
        ]

    a2a = [slab_copies(0), slab_copies(1)]

    for j in range(1, N):
        @pl.when(d >= j)
        def _(j=j):
            a2a[0][N - j - 1].start()

    for j in range(1, N):
        @pl.when(d + j < N)
        def _(j=j):
            pl.semaphore_wait(answer.at[j - 1], 1)
            a2a[0][j - 1].start()

    @pl.when(core == 0)
    def _():
        for copy in a2a[1]:
            copy.start()

    for copy in args:
        copy.wait()
    load.wait()
    first = (r * N + d) * n

    def pick(i, carry):
        base = pl.multiple_of(i * 8, 8)
        rows = []
        for j in range(8):
            local = head_ids[base + j] - first
            owned = jnp.logical_and(local >= 0, local < n)
            row = tab[pl.ds(jnp.clip(local, 0, n - 1), 1), :]
            rows.append(jnp.where(owned, row, jnp.zeros_like(row)))
        part[pl.ds(base, 8), :] = jnp.concatenate(rows, axis=0)
        return carry

    lax.fori_loop(0, Q // 8, pick, 0)

    def remote(src, dst, sems, at, peer):
        return pltpu.make_async_remote_copy(
            src_ref=src, dst_ref=dst, send_sem=sems[0].at[at], recv_sem=sems[1].at[at],
            device_id=peer, device_id_type=MESH,
        )

    def add_rows(h, dst, dst_at, src, src_at, extra, extra_at):
        rows = min(64, h)

        def add(i, carry):
            step = i * rows
            dst[pl.ds(pl.multiple_of(dst_at + step, 8), rows), :] = (
                src[pl.ds(pl.multiple_of(src_at + step, 8), rows), :]
                + extra[pl.ds(pl.multiple_of(extra_at + step, 8), rows), :]
            )
            return carry

        lax.fori_loop(0, h // rows, add, 0)

    for b, (bit, other) in enumerate(row_pairs):
        @pl.when(bit == 0)
        def _(b=b):
            pl.semaphore_wait(answer.at[N - 1 + b], 1)

    row_bits = list(range(nrow))
    orders = [row_bits, row_bits[:1] + row_bits[:0:-1]]
    ex = (ex_send, ex_recv)

    offset = [0, half_q]
    size = half_q
    into = 0
    for k in range(nrow):
        h = size // 2
        copies = []
        for s in range(2):
            bit, other = bit_and_other(r, orders[s][k])
            gone = pl.multiple_of(offset[s] + (1 - bit) * h, 8)
            copy = remote(
                part.at[pl.ds(gone, h), :],
                recv.at[pl.ds(s * half_q + into, h), :],
                ex, (s, k), (other, d),
            )
            copy.start()
            copies.append(copy)
            offset[s] = pl.multiple_of(offset[s] + bit * h, 8)
        if k == 0:
            def narrow(i, carry):
                at = pl.multiple_of(i * 128, 128)
                low[pl.ds(at, 128), :] = tab[pl.ds(at, 128), :].astype(jnp.bfloat16)
                return carry

            lax.fori_loop(0, n // 128, narrow, 0)
        if k == 1:
            idx = thr_idx[...]

            def choose(t, acc):
                return jnp.where(idx == t, thr[t], acc)

            lev[...] = lax.fori_loop(0, thr.shape[0], choose, jnp.zeros(idx.shape, jnp.float32))
        for s in range(2):
            copies[s].wait()
            if k < nrow - 1:
                add_rows(h, part, offset[s], part, offset[s], recv, s * half_q + into)
            else:
                add_rows(h, zsum, (2 * s + core) * h, part, offset[s], recv, s * half_q + into)
        into += h
        size = h

    partner = (r + 1 - 2 * core, d)
    skip = half_q // 2
    core0_at = [pl.multiple_of(offset[s] - core * skip, 8) for s in range(2)]
    pair = (pair_send, pair_recv)
    there_ = [
        remote(zsum.at[pl.ds(2 * s * size, size), :], zsum.at[pl.ds(2 * s * size, size), :], pair, (0, s), partner)
        for s in range(2)
    ]
    back = [
        remote(zout.at[pl.ds(2 * s * size, size), :], full.at[pl.ds(core0_at[s], size), :], pair, (1, s), partner)
        for s in range(2)
    ]
    zx = (z_send, z_recv)

    @pl.when(core == 0)
    def _():
        for copy in there_:
            copy.start()
        for copy in there_:
            copy.wait_send()
        for copy in back:
            copy.wait_recv()

    @pl.when(core == 1)
    def _():
        for copy in there_:
            copy.wait_recv()
        at, count_, into = 0, 4 * size, 0
        for b in range(ndim):
            h = count_ // 2
            bit, other = bit_and_other(d, b)
            gone = pl.multiple_of(at + (1 - bit) * h, 8)
            copy = remote(zsum.at[pl.ds(gone, h), :], zin.at[pl.ds(into, h), :], zx, b, (r, other))
            copy.start()
            at = pl.multiple_of(at + bit * h, 8)
            copy.wait()
            add_rows(h, zsum, at, zsum, at, zin, into)
            into += h
            count_ = h

        def form(i, carry):
            z = pl.multiple_of(at + i * 8, 8)
            slot = z // size
            s = slot // 2
            c = slot - 2 * s
            q = (1 - s) * core0_at[0] + s * core0_at[1] + c * skip + (z - slot * size)
            rows = [rel[pl.ds(rel_ids[q + j], 1), :] for j in range(8)]
            zout[pl.ds(z, 8), :] = zsum[pl.ds(z, 8), :] * jnp.concatenate(rows, axis=0)
            return carry

        lax.fori_loop(0, count_ // 8, form, 0)
        for b in reversed(range(ndim)):
            bit, other = bit_and_other(d, b)
            here = zout.at[pl.ds(at, count_), :]
            copy = remote(here, here, zx, ndim + b, (r, other))
            copy.start()
            if b == 0:
                for late in a2a[1]:
                    late.start()
            copy.wait()
            at = pl.multiple_of(at - bit * count_, 8)
            count_ = 2 * count_
        for copy in back:
            copy.start()
        for s in range(2):
            rows = min(64, size)

            def take(i, carry, s=s):
                step = i * rows
                full[pl.ds(pl.multiple_of(offset[s] + step, 8), rows), :] = (
                    zout[pl.ds(pl.multiple_of((2 * s + 1) * size + step, 8), rows), :]
                )
                return carry

            lax.fori_loop(0, size // rows, take, 0)
        for copy in back:
            copy.wait_send()

    def count_pair(q0, q1):
        qb[:lanes, :] = full[pl.ds(q0, lanes), :].astype(jnp.bfloat16)
        qb[lanes:, :] = full[pl.ds(q1, lanes), :].astype(jnp.bfloat16)
        i0 = q0 // lanes
        i1 = q1 // lanes
        level = jnp.concatenate([lev[i0], lev[i1]], axis=1)
        rows = 512

        def tile(i, acc):
            at = pl.multiple_of(i * rows, rows)
            score = lax.dot_general(
                low[pl.ds(at, rows), :], qb[...], (((1,), (1,)), ((), ())),
                preferred_element_type=jnp.float32,
            )
            soft = jax.nn.sigmoid(sharpness * (score - level))
            return acc + jnp.sum(soft.reshape(rows // 8, 8, 2 * lanes), axis=0)

        acc = lax.fori_loop(0, n // rows, tile, jnp.zeros((8, 2 * lanes), jnp.float32))
        share = jnp.sum(acc, axis=0, keepdims=True) * (1.0 / total_ents)
        frac[i0] = share[:, :lanes]
        frac[i1] = share[:, lanes:]

    def count(starts_, rows):
        def body(i, carry):
            count_pair(pl.multiple_of(starts_[0] + i * lanes, lanes), pl.multiple_of(starts_[1] + i * lanes, lanes))
            return carry

        lax.fori_loop(0, rows // lanes, body, 0)

    pending = None
    counted = False
    if size >= lanes:
        pending = (list(offset), size)
        counted = True
    for k in reversed(range(nrow)):
        copies = []
        there = []
        for s in range(2):
            bit, other = bit_and_other(r, orders[s][k])
            here = full.at[pl.ds(offset[s], size), :]
            copy = remote(here, here, ex, (s, nrow + k), (other, d))
            copy.start()
            copies.append(copy)
            there.append(pl.multiple_of(offset[s] + (1 - 2 * bit) * size, 8))
            offset[s] = pl.multiple_of(offset[s] - bit * size, 8)
        if pending is not None:
            count(*pending)
            pending = None
        for copy in copies:
            copy.wait()
        size = 2 * size
        if size >= lanes:
            pending = (there, size // 2) if counted else (list(offset), size)
            counted = True
    count(*pending)

    per = frac.shape[0] // R
    fx = (f_send, f_recv)
    handed = remote(frac, fr_pair, fx, 0, partner)
    last = remote(fr_all, fr_all, (last_send, last_recv), 0, partner)

    @pl.when(core == 1)
    def _():
        handed.start()
        handed.wait_send()
        last.wait_recv()

    @pl.when(core == 0)
    def _():
        handed.wait_recv()
        frac[...] = frac[...] + fr_pair[...]
        at, held, into = 0, frac.shape[0], 0
        for b in reversed(range(1, nrow)):
            h = held // 2
            bit, other = bit_and_other(r, b)
            copy = remote(frac.at[pl.ds(at + (1 - bit) * h, h)], fr_in.at[pl.ds(into, h)], fx, b, (other, d))
            copy.start()
            at = at + bit * h
            copy.wait()
            frac[pl.ds(at, h)] = frac[pl.ds(at, h)] + fr_in[pl.ds(into, h)]
            into += h
            held = h
        total = frac[pl.ds(at, held)]
        fr_sum[...] = total
        sends = []
        for k, t in enumerate(dim_peers):
            copy = pltpu.make_async_remote_copy(
                src_ref=fr_sum, dst_ref=fr_dim.at[k],
                send_sem=g_send.at[k], recv_sem=g_recv.at[k],
                device_id=(r, t), device_id_type=MESH,
            )
            copy.start()
            sends.append(copy)
        for k in range(N - 1):
            sends[k].wait()
            total = total + fr_dim[k]
        fr_all[...] = total
        last.start()
        last.wait_send()

    mine = frac_out.shape[1]
    row = fr_all[core * per + d * mine // lanes]
    place = lax.rem(d * mine, lanes) // mine
    out = row[:, :mine]
    for j in range(1, lanes // mine):
        out = jnp.where(place == j, row[:, j * mine:(j + 1) * mine], out)
    frac_out[...] = out
    own.wait()
    for copies in a2a:
        for copy in copies:
            copy.wait()


def place(parts, serving, share, serving_out, share_out, sems):
    rows = serving.shape[0] // parts
    copies = [
        pltpu.make_async_copy(
            serving.at[pl.ds(i * rows, rows), :], serving_out.at[pl.ds(i * rows, rows), :], sems.at[i]
        )
        for i in range(parts)
    ]
    copies.append(pltpu.make_async_copy(share, share_out, sems.at[parts]))
    for copy in copies:
        copy.start()
    for copy in copies:
        copy.wait()


def shards(entity_table, relations, thresholds, head_ids, rel_ids, thr_idx):
    R = lax.axis_size("rows")
    N = lax.axis_size("dim")
    n, width = entity_table.shape
    Q = head_ids.shape[0]
    blocks = Q // lanes
    per = blocks // R
    group = 2 * Q // R
    f32 = jnp.float32
    DMA = pltpu.SemaphoreType.DMA
    vmem = pl.BlockSpec(memory_space=pltpu.VMEM)
    hbm = pl.BlockSpec(memory_space=pltpu.HBM)
    anywhere = pl.BlockSpec(memory_space=pl.ANY)
    mine = Q // (R * N)
    operands = [head_ids, rel_ids, thresholds, thr_idx.reshape(blocks, 1, lanes), relations, entity_table]
    if (width // N) % lanes:
        operands.append(entity_table.reshape(n, N, width // N).transpose(1, 0, 2))
    serving, share = pl.pallas_call(
        functools.partial(kernel, R, N, n * R * N),
        out_shape=(
            pltpu.VMEM((n * N, width // N), f32),
            jax.ShapeDtypeStruct((1, mine), f32),
        ),
        in_specs=[hbm] * len(operands),
        out_specs=(anywhere, vmem),
        scratch_shapes=[
            pltpu.SMEM((Q,), jnp.int32),
            pltpu.SMEM((Q,), jnp.int32),
            pltpu.SMEM(thresholds.shape, f32),
            pltpu.VMEM((blocks, 1, lanes), jnp.int32),
            pltpu.VMEM(relations.shape, f32),
            DMA((5,)),
            pltpu.VMEM((n, width), f32),
            pltpu.VMEM((n, width), jnp.bfloat16),
            pltpu.VMEM((Q, width), f32),
            pltpu.VMEM((Q, width), f32),
            pltpu.VMEM((Q, width), f32),
            pltpu.VMEM((group, width), f32),
            pltpu.VMEM((group, width), f32),
            pltpu.VMEM((group, width), f32),
            pltpu.VMEM((2 * lanes, width), jnp.bfloat16),
            pltpu.VMEM((blocks, 1, lanes), f32),
            pltpu.VMEM((blocks, 1, lanes), f32),
            pltpu.VMEM((blocks, 1, lanes), f32),
            pltpu.VMEM((blocks, 1, lanes), f32),
            pltpu.VMEM((N - 1, 2 * per, 1, lanes), f32),
            pltpu.VMEM((2 * per, 1, lanes), f32),
            pltpu.VMEM((2 * per, 1, lanes), f32),
            DMA, DMA,
            DMA((2, N - 1)), DMA((2, N - 1)),
            DMA((2, 2 * bits_of(R))), DMA((2, 2 * bits_of(R))),
            DMA((2 * bits_of(N),)), DMA((2 * bits_of(N),)),
            DMA((2, 2)), DMA((2, 2)),
            DMA((bits_of(R),)), DMA((bits_of(R),)),
            DMA((N - 1,)), DMA((N - 1,)),
            DMA((1,)), DMA((1,)),
            pltpu.SemaphoreType.REGULAR((N - 1 + bits_of(R),)),
        ],
        compiler_params=pltpu.CompilerParams(
            collective_id=0, has_side_effects=True, vmem_limit_bytes=40 * 2**20
        ),
    )(*[pltpu.with_memory_space_constraint(x, pltpu.HBM) for x in operands])
    parts = 8
    serving, share = pl.pallas_call(
        functools.partial(place, parts),
        out_shape=(
            jax.ShapeDtypeStruct(serving.shape, f32),
            jax.ShapeDtypeStruct(share.shape, f32),
        ),
        in_specs=[vmem] * 2,
        out_specs=(anywhere, anywhere),
        scratch_shapes=[DMA((parts + 1,))],
        compiler_params=pltpu.CompilerParams(vmem_limit_bytes=4 * 2**20),
    )(*[pltpu.with_memory_space_constraint(x, pltpu.VMEM) for x in (serving, share)])
    return serving, share.reshape(mine)


def solution(mesh):
    placed = (P(("rows", "dim"), None), P(), P(), P(), P(), P())
    return jax.shard_map(
        shards,
        mesh=mesh,
        in_specs=placed,
        out_specs=(P("rows", "dim"), P(("rows", "dim"))),
        check_vma=False,
    )
```

```python
import functools
import jax
import jax.numpy as jnp
from jax import lax
from jax.sharding import PartitionSpec as P
from jax.experimental import pallas as pl
from jax.experimental.pallas import tpu as pltpu

MESH = pl.DeviceIdType.MESH
sharpness = 2.0
lanes = 128
units = 16
entry = 3


def bits_of(size):
    assert size & (size - 1) == 0
    return size.bit_length() - 1


def kernel(
    R, N, total_ents, head_ids_, rel_ids_, thr_, thr_idx_, rel_, table, *others
):
    slabs = others[:-41]
    (
        serving, frac_out,
        head_ids, rel_ids, thr, thr_idx, rel, arg_sem,
        tab, low, part, recv, full, zsum, zin, zout, qb, lev, frac, fr_pair, fr_in, fr_dim, fr_sum, fr_all,
        load_sem, own_sem, a2a_send, a2a_recv, ex_send, ex_recv, z_send, z_recv,
        pair_send, pair_recv, f_send, f_recv, g_send, g_recv, last_send, last_recv, answer,
    ) = others[-41:]
    r = lax.axis_index("rows")
    d = lax.axis_index("dim")
    core = lax.rem(r, 2)
    n, width = table.shape
    slab = width // N
    Q = part.shape[0]
    half_q = Q // 2
    nrow = bits_of(R)
    ndim = bits_of(N)

    def slab_rows(t, start, rows):
        if slabs:
            return slabs[0].at[t, pl.ds(start, rows), :]
        return table.at[pl.ds(start, rows), pl.ds(pl.multiple_of(t * slab, slab), slab)]

    def bit_and_other(me, b):
        bit = lax.rem(me // (2 ** b), 2)
        return bit, me + (1 - 2 * bit) * (2 ** b)

    dim_peers = []
    for k in range(1, N):
        t = d
        for b in range(ndim):
            if k // 2 ** b % 2:
                t = t + (bit_and_other(d, b)[1] - d)
        dim_peers.append(t)
    def ahead(j):
        return (r, lax.rem(d + j, N)), d + j < N

    def behind(j):
        return (r, lax.rem(d + N - j, N)), d >= j

    row_pairs = [bit_and_other(r, b) for b in range(nrow)]
    barrier = pltpu.get_barrier_semaphore()
    leaders = d
    for j in range(1, N):
        peer, leads = ahead(j)

        @pl.when(leads)
        def _(peer=peer):
            pl.semaphore_signal(barrier, inc=1, device_id=peer, device_id_type=MESH)

    for bit, other in row_pairs:
        leaders = leaders + bit

        @pl.when(bit == 0)
        def _(other=other):
            pl.semaphore_signal(barrier, inc=1, device_id=(other, d), device_id_type=MESH)


    @pl.when(leaders > 0)
    def _():
        pl.semaphore_wait(barrier, leaders)

    for j in range(1, N):
        peer, follows = behind(j)

        @pl.when(follows)
        def _(j=j, peer=peer):
            pl.semaphore_signal(answer.at[j - 1], inc=1, device_id=peer, device_id_type=MESH)

    for b, (bit, other) in enumerate(row_pairs):
        @pl.when(bit == 1)
        def _(b=b, other=other):
            pl.semaphore_signal(answer.at[N - 1 + b], inc=1, device_id=(other, d), device_id_type=MESH)

    first_rows = n * entry // units

    def slab_copies(piece):
        start, rows = ((0, first_rows), (first_rows, n - first_rows))[piece]
        return [
            pltpu.make_async_remote_copy(
                src_ref=slab_rows(t, start, rows),
                dst_ref=serving.at[pl.ds(pl.multiple_of(d * n + start, 8), rows), :],
                send_sem=a2a_send.at[piece, k],
                recv_sem=a2a_recv.at[piece, k],
                device_id=(r, t),
                device_id_type=MESH,
            )
            for k, t in enumerate(dim_peers if piece else [lax.rem(d + j, N) for j in range(1, N)])
        ]

    a2a = [slab_copies(0), slab_copies(1)]

    for j in range(1, N):
        @pl.when(d >= j)
        def _(j=j):
            a2a[0][N - j - 1].start()

    load = pltpu.make_async_copy(table, tab, load_sem)
    load.start()
    own = pltpu.make_async_copy(
        slab_rows(d, 0, n),
        serving.at[pl.ds(pl.multiple_of(d * n, 8), n), :],
        own_sem,
    )
    own.start()
    pairs = [(head_ids_, head_ids), (rel_ids_, rel_ids), (thr_, thr), (thr_idx_, thr_idx), (rel_, rel)]
    args = [pltpu.make_async_copy(src, dst, arg_sem.at[i]) for i, (src, dst) in enumerate(pairs)]
    for copy in args:
        copy.start()

    for j in range(1, N):
        @pl.when(d + j < N)
        def _(j=j):
            pl.semaphore_wait(answer.at[j - 1], 1)
            a2a[0][j - 1].start()

    @pl.when(core == 0)
    def _():
        for copy in a2a[1]:
            copy.start()

    for copy in args:
        copy.wait()
    load.wait()
    first = (r * N + d) * n

    def pick(i, carry):
        base = pl.multiple_of(i * 8, 8)
        rows = []
        for j in range(8):
            local = head_ids[base + j] - first
            owned = jnp.logical_and(local >= 0, local < n)
            row = tab[pl.ds(jnp.clip(local, 0, n - 1), 1), :]
            rows.append(jnp.where(owned, row, jnp.zeros_like(row)))
        part[pl.ds(base, 8), :] = jnp.concatenate(rows, axis=0)
        return carry

    lax.fori_loop(0, Q // 8, pick, 0)

    def remote(src, dst, sems, at, peer):
        return pltpu.make_async_remote_copy(
            src_ref=src, dst_ref=dst, send_sem=sems[0].at[at], recv_sem=sems[1].at[at],
            device_id=peer, device_id_type=MESH,
        )

    def add_rows(h, dst, dst_at, src, src_at, extra, extra_at):
        rows = min(64, h)

        def add(i, carry):
            step = i * rows
            dst[pl.ds(pl.multiple_of(dst_at + step, 8), rows), :] = (
                src[pl.ds(pl.multiple_of(src_at + step, 8), rows), :]
                + extra[pl.ds(pl.multiple_of(extra_at + step, 8), rows), :]
            )
            return carry

        lax.fori_loop(0, h // rows, add, 0)

    for b, (bit, other) in enumerate(row_pairs):
        @pl.when(bit == 0)
        def _(b=b):
            pl.semaphore_wait(answer.at[N - 1 + b], 1)

    row_bits = list(range(nrow))
    orders = [row_bits, row_bits[:1] + row_bits[:0:-1]]
    ex = (ex_send, ex_recv)

    offset = [0, half_q]
    size = half_q
    into = 0
    for k in range(nrow):
        h = size // 2
        copies = []
        for s in range(2):
            bit, other = bit_and_other(r, orders[s][k])
            gone = pl.multiple_of(offset[s] + (1 - bit) * h, 8)
            copy = remote(
                part.at[pl.ds(gone, h), :],
                recv.at[pl.ds(s * half_q + into, h), :],
                ex, (s, k), (other, d),
            )
            copy.start()
            copies.append(copy)
            offset[s] = pl.multiple_of(offset[s] + bit * h, 8)
        if k == 0:
            def narrow(i, carry):
                at = pl.multiple_of(i * 128, 128)
                low[pl.ds(at, 128), :] = tab[pl.ds(at, 128), :].astype(jnp.bfloat16)
                return carry

            lax.fori_loop(0, n // 128, narrow, 0)
        if k == min(1, nrow - 1):
            idx = thr_idx[...]

            def choose(t, acc):
                return jnp.where(idx == t, thr[t], acc)

            lev[...] = lax.fori_loop(0, thr.shape[0], choose, jnp.zeros(idx.shape, jnp.float32))
        for s in range(2):
            copies[s].wait()
            if k < nrow - 1:
                add_rows(h, part, offset[s], part, offset[s], recv, s * half_q + into)
            else:
                add_rows(h, zsum, (2 * s + core) * h, part, offset[s], recv, s * half_q + into)
        into += h
        size = h

    partner = (r + 1 - 2 * core, d)
    skip = half_q // 2
    core0_at = [pl.multiple_of(offset[s] - core * skip, 8) for s in range(2)]
    pair = (pair_send, pair_recv)
    there_ = [
        remote(zsum.at[pl.ds(2 * s * size, size), :], zsum.at[pl.ds(2 * s * size, size), :], pair, (0, s), partner)
        for s in range(2)
    ]
    back = [
        remote(zout.at[pl.ds(2 * s * size, size), :], full.at[pl.ds(core0_at[s], size), :], pair, (1, s), partner)
        for s in range(2)
    ]
    zx = (z_send, z_recv)

    @pl.when(core == 0)
    def _():
        for copy in there_:
            copy.start()
        for copy in there_:
            copy.wait_send()
        for copy in back:
            copy.wait_recv()

    @pl.when(core == 1)
    def _():
        for copy in there_:
            copy.wait_recv()
        at, count_, into = 0, 4 * size, 0
        for b in range(ndim):
            h = count_ // 2
            bit, other = bit_and_other(d, b)
            gone = pl.multiple_of(at + (1 - bit) * h, 8)
            copy = remote(zsum.at[pl.ds(gone, h), :], zin.at[pl.ds(into, h), :], zx, b, (r, other))
            copy.start()
            at = pl.multiple_of(at + bit * h, 8)
            copy.wait()
            add_rows(h, zsum, at, zsum, at, zin, into)
            into += h
            count_ = h

        def form(i, carry):
            z = pl.multiple_of(at + i * 8, 8)
            slot = z // size
            s = slot // 2
            c = slot - 2 * s
            q = (1 - s) * core0_at[0] + s * core0_at[1] + c * skip + (z - slot * size)
            rows = [rel[pl.ds(rel_ids[q + j], 1), :] for j in range(8)]
            zout[pl.ds(z, 8), :] = zsum[pl.ds(z, 8), :] * jnp.concatenate(rows, axis=0)
            return carry

        lax.fori_loop(0, count_ // 8, form, 0)
        for b in reversed(range(ndim)):
            bit, other = bit_and_other(d, b)
            here = zout.at[pl.ds(at, count_), :]
            copy = remote(here, here, zx, ndim + b, (r, other))
            copy.start()
            if b == 0:
                for late in a2a[1]:
                    late.start()
            copy.wait()
            at = pl.multiple_of(at - bit * count_, 8)
            count_ = 2 * count_
        for copy in back:
            copy.start()
        for s in range(2):
            rows = min(64, size)

            def take(i, carry, s=s):
                step = i * rows
                full[pl.ds(pl.multiple_of(offset[s] + step, 8), rows), :] = (
                    zout[pl.ds(pl.multiple_of((2 * s + 1) * size + step, 8), rows), :]
                )
                return carry

            lax.fori_loop(0, size // rows, take, 0)
        for copy in back:
            copy.wait_send()

    def count_pair(q0, q1):
        qb[:lanes, :] = full[pl.ds(q0, lanes), :].astype(jnp.bfloat16)
        qb[lanes:, :] = full[pl.ds(q1, lanes), :].astype(jnp.bfloat16)
        i0 = q0 // lanes
        i1 = q1 // lanes
        level = jnp.concatenate([lev[i0], lev[i1]], axis=1)
        rows = 512

        def tile(i, acc):
            at = pl.multiple_of(i * rows, rows)
            score = lax.dot_general(
                low[pl.ds(at, rows), :], qb[...], (((1,), (1,)), ((), ())),
                preferred_element_type=jnp.float32,
            )
            soft = jax.nn.sigmoid(sharpness * (score - level))
            return acc + jnp.sum(soft.reshape(rows // 8, 8, 2 * lanes), axis=0)

        acc = lax.fori_loop(0, n // rows, tile, jnp.zeros((8, 2 * lanes), jnp.float32))
        share = jnp.sum(acc, axis=0, keepdims=True) * (1.0 / total_ents)
        frac[i0] = share[:, :lanes]
        frac[i1] = share[:, lanes:]

    def count(starts_, rows):
        def body(i, carry):
            count_pair(pl.multiple_of(starts_[0] + i * lanes, lanes), pl.multiple_of(starts_[1] + i * lanes, lanes))
            return carry

        lax.fori_loop(0, rows // lanes, body, 0)

    pending = None
    counted = False
    if size >= lanes:
        pending = (list(offset), size)
        counted = True
    for k in reversed(range(nrow)):
        copies = []
        there = []
        for s in range(2):
            bit, other = bit_and_other(r, orders[s][k])
            here = full.at[pl.ds(offset[s], size), :]
            copy = remote(here, here, ex, (s, nrow + k), (other, d))
            copy.start()
            copies.append(copy)
            there.append(pl.multiple_of(offset[s] + (1 - 2 * bit) * size, 8))
            offset[s] = pl.multiple_of(offset[s] - bit * size, 8)
        if pending is not None:
            count(*pending)
            pending = None
        for copy in copies:
            copy.wait()
        size = 2 * size
        if size >= lanes:
            pending = (there, size // 2) if counted else (list(offset), size)
            counted = True
    count(*pending)

    per = frac.shape[0] // R
    fx = (f_send, f_recv)
    handed = remote(frac, fr_pair, fx, 0, partner)
    last = remote(fr_all, fr_all, (last_send, last_recv), 0, partner)

    @pl.when(core == 1)
    def _():
        handed.start()
        handed.wait_send()
        last.wait_recv()

    @pl.when(core == 0)
    def _():
        handed.wait_recv()
        frac[...] = frac[...] + fr_pair[...]
        at, held, into = 0, frac.shape[0], 0
        for b in reversed(range(1, nrow)):
            h = held // 2
            bit, other = bit_and_other(r, b)
            copy = remote(frac.at[pl.ds(at + (1 - bit) * h, h)], fr_in.at[pl.ds(into, h)], fx, b, (other, d))
            copy.start()
            at = at + bit * h
            copy.wait()
            frac[pl.ds(at, h)] = frac[pl.ds(at, h)] + fr_in[pl.ds(into, h)]
            into += h
            held = h
        total = frac[pl.ds(at, held)]
        fr_sum[...] = total
        sends = []
        for k, t in enumerate(dim_peers):
            copy = pltpu.make_async_remote_copy(
                src_ref=fr_sum, dst_ref=fr_dim.at[k],
                send_sem=g_send.at[k], recv_sem=g_recv.at[k],
                device_id=(r, t), device_id_type=MESH,
            )
            copy.start()
            sends.append(copy)
        for k in range(N - 1):
            sends[k].wait()
            total = total + fr_dim[k]
        fr_all[...] = total
        last.start()
        last.wait_send()

    mine = frac_out.shape[1]
    row = fr_all[core * per + d * mine // lanes]
    place = lax.rem(d * mine, lanes) // mine
    out = row[:, :mine]
    for j in range(1, lanes // mine):
        out = jnp.where(place == j, row[:, j * mine:(j + 1) * mine], out)
    frac_out[...] = out
    own.wait()
    for copies in a2a:
        for copy in copies:
            copy.wait()


def place(parts, serving, share, serving_out, share_out, sems):
    rows = serving.shape[0] // parts
    copies = [
        pltpu.make_async_copy(
            serving.at[pl.ds(i * rows, rows), :], serving_out.at[pl.ds(i * rows, rows), :], sems.at[i]
        )
        for i in range(parts)
    ]
    copies.append(pltpu.make_async_copy(share, share_out, sems.at[parts]))
    for copy in copies:
        copy.start()
    for copy in copies:
        copy.wait()


def shards(entity_table, relations, thresholds, head_ids, rel_ids, thr_idx):
    R = lax.axis_size("rows")
    N = lax.axis_size("dim")
    n, width = entity_table.shape
    Q = head_ids.shape[0]
    blocks = Q // lanes
    per = blocks // R
    group = 2 * Q // R
    f32 = jnp.float32
    DMA = pltpu.SemaphoreType.DMA
    vmem = pl.BlockSpec(memory_space=pltpu.VMEM)
    hbm = pl.BlockSpec(memory_space=pltpu.HBM)
    anywhere = pl.BlockSpec(memory_space=pl.ANY)
    mine = Q // (R * N)
    operands = [head_ids, rel_ids, thresholds, thr_idx.reshape(blocks, 1, lanes), relations, entity_table]
    if (width // N) % lanes:
        operands.append(entity_table.reshape(n, N, width // N).transpose(1, 0, 2))
    serving, share = pl.pallas_call(
        functools.partial(kernel, R, N, n * R * N),
        out_shape=(
            pltpu.VMEM((n * N, width // N), f32),
            jax.ShapeDtypeStruct((1, mine), f32),
        ),
        in_specs=[hbm] * len(operands),
        out_specs=(anywhere, vmem),
        scratch_shapes=[
            pltpu.SMEM((Q,), jnp.int32),
            pltpu.SMEM((Q,), jnp.int32),
            pltpu.SMEM(thresholds.shape, f32),
            pltpu.VMEM((blocks, 1, lanes), jnp.int32),
            pltpu.VMEM(relations.shape, f32),
            DMA((5,)),
            pltpu.VMEM((n, width), f32),
            pltpu.VMEM((n, width), jnp.bfloat16),
            pltpu.VMEM((Q, width), f32),
            pltpu.VMEM((Q, width), f32),
            pltpu.VMEM((Q, width), f32),
            pltpu.VMEM((group, width), f32),
            pltpu.VMEM((group, width), f32),
            pltpu.VMEM((group, width), f32),
            pltpu.VMEM((2 * lanes, width), jnp.bfloat16),
            pltpu.VMEM((blocks, 1, lanes), f32),
            pltpu.VMEM((blocks, 1, lanes), f32),
            pltpu.VMEM((blocks, 1, lanes), f32),
            pltpu.VMEM((blocks, 1, lanes), f32),
            pltpu.VMEM((N - 1, 2 * per, 1, lanes), f32),
            pltpu.VMEM((2 * per, 1, lanes), f32),
            pltpu.VMEM((2 * per, 1, lanes), f32),
            DMA, DMA,
            DMA((2, N - 1)), DMA((2, N - 1)),
            DMA((2, 2 * bits_of(R))), DMA((2, 2 * bits_of(R))),
            DMA((2 * bits_of(N),)), DMA((2 * bits_of(N),)),
            DMA((2, 2)), DMA((2, 2)),
            DMA((bits_of(R),)), DMA((bits_of(R),)),
            DMA((N - 1,)), DMA((N - 1,)),
            DMA((1,)), DMA((1,)),
            pltpu.SemaphoreType.REGULAR((N - 1 + bits_of(R),)),
        ],
        compiler_params=pltpu.CompilerParams(
            collective_id=0, has_side_effects=True, vmem_limit_bytes=40 * 2**20
        ),
    )(*[pltpu.with_memory_space_constraint(x, pltpu.HBM) for x in operands])
    parts = 8
    serving, share = pl.pallas_call(
        functools.partial(place, parts),
        out_shape=(
            jax.ShapeDtypeStruct(serving.shape, f32),
            jax.ShapeDtypeStruct(share.shape, f32),
        ),
        in_specs=[vmem] * 2,
        out_specs=(anywhere, anywhere),
        scratch_shapes=[DMA((parts + 1,))],
        compiler_params=pltpu.CompilerParams(vmem_limit_bytes=4 * 2**20),
    )(*[pltpu.with_memory_space_constraint(x, pltpu.VMEM) for x in (serving, share)])
    return serving, share.reshape(mine)


def solution(mesh):
    placed = (P(("rows", "dim"), None), P(), P(), P(), P(), P())
    return jax.shard_map(
        shards,
        mesh=mesh,
        in_specs=placed,
        out_specs=(P("rows", "dim"), P(("rows", "dim"))),
        check_vma=False,
    )
```

```python
import functools
import jax
import jax.numpy as jnp
from jax import lax
from jax.sharding import PartitionSpec as P
from jax.experimental import pallas as pl
from jax.experimental.pallas import tpu as pltpu

MESH = pl.DeviceIdType.MESH
sharpness = 2.0
lanes = 128
units = 16
entry = 3


def bits_of(size):
    assert size & (size - 1) == 0
    return size.bit_length() - 1


def kernel(
    R, N, total_ents, head_ids_, rel_ids_, thr_, thr_idx_, rel_, table, *others
):
    slabs = others[:-42]
    (
        serving, frac_out,
        head_ids, rel_ids, thr, thr_idx, rel, arg_sem,
        tab, low, part, recv, full, zsum, zin, zout, qb, lev, frac, fr_pair, fr_in, fr_dim, fr_sum, fr_all,
        load_sem, own_sem, a2a_send, a2a_recv, ex_send, ex_recv, z_send, z_recv,
        pair_send, pair_recv, f_send, f_recv, g_send, g_recv, last_send, last_recv, answer, word,
    ) = others[-42:]
    r = lax.axis_index("rows")
    d = lax.axis_index("dim")
    core = lax.rem(r, 2)
    n, width = table.shape
    slab = width // N
    Q = part.shape[0]
    half_q = Q // 2
    nrow = bits_of(R)
    ndim = bits_of(N)

    def slab_rows(t, start, rows):
        if slabs:
            return slabs[0].at[t, pl.ds(start, rows), :]
        return table.at[pl.ds(start, rows), pl.ds(pl.multiple_of(t * slab, slab), slab)]

    def bit_and_other(me, b):
        bit = lax.rem(me // (2 ** b), 2)
        return bit, me + (1 - 2 * bit) * (2 ** b)

    dim_peers = []
    for k in range(1, N):
        t = d
        for b in range(ndim):
            if k // 2 ** b % 2:
                t = t + (bit_and_other(d, b)[1] - d)
        dim_peers.append(t)
    def ahead(j):
        return (r, lax.rem(d + j, N)), d + j < N

    def behind(j):
        return (r, lax.rem(d + N - j, N)), d >= j

    row_pairs = [bit_and_other(r, b) for b in range(nrow)]
    barrier = pltpu.get_barrier_semaphore()
    leaders = d
    for j in range(1, N):
        peer, leads = ahead(j)

        @pl.when(leads)
        def _(peer=peer):
            pl.semaphore_signal(barrier, inc=1, device_id=peer, device_id_type=MESH)

    at_head = d == 0
    for bit, other in row_pairs:
        leaders = leaders + jnp.where(at_head, bit, 0)

        @pl.when(jnp.logical_and(at_head, bit == 0))
        def _(other=other):
            pl.semaphore_signal(barrier, inc=1, device_id=(other, d), device_id_type=MESH)


    @pl.when(leaders > 0)
    def _():
        pl.semaphore_wait(barrier, leaders)

    for j in range(1, N):
        peer, follows = behind(j)

        @pl.when(follows)
        def _(j=j, peer=peer):
            pl.semaphore_signal(answer.at[j - 1], inc=1, device_id=peer, device_id_type=MESH)

    for b, (bit, other) in enumerate(row_pairs):
        @pl.when(jnp.logical_and(at_head, bit == 1))
        def _(b=b, other=other):
            pl.semaphore_signal(answer.at[N - 1 + b], inc=1, device_id=(other, d), device_id_type=MESH)

    first_rows = n * entry // units

    def slab_copies(piece):
        start, rows = ((0, first_rows), (first_rows, n - first_rows))[piece]
        return [
            pltpu.make_async_remote_copy(
                src_ref=slab_rows(t, start, rows),
                dst_ref=serving.at[pl.ds(pl.multiple_of(d * n + start, 8), rows), :],
                send_sem=a2a_send.at[piece, k],
                recv_sem=a2a_recv.at[piece, k],
                device_id=(r, t),
                device_id_type=MESH,
            )
            for k, t in enumerate(dim_peers if piece else [lax.rem(d + j, N) for j in range(1, N)])
        ]

    a2a = [slab_copies(0), slab_copies(1)]

    for j in range(1, N):
        @pl.when(d >= j)
        def _(j=j):
            a2a[0][N - j - 1].start()

    load = pltpu.make_async_copy(table, tab, load_sem)
    load.start()
    own = pltpu.make_async_copy(
        slab_rows(d, 0, n),
        serving.at[pl.ds(pl.multiple_of(d * n, 8), n), :],
        own_sem,
    )
    own.start()
    pairs = [(head_ids_, head_ids), (rel_ids_, rel_ids), (thr_, thr), (thr_idx_, thr_idx), (rel_, rel)]
    args = [pltpu.make_async_copy(src, dst, arg_sem.at[i]) for i, (src, dst) in enumerate(pairs)]
    for copy in args:
        copy.start()

    for j in range(1, N):
        @pl.when(d + j < N)
        def _(j=j):
            pl.semaphore_wait(answer.at[j - 1], 1)
            a2a[0][j - 1].start()

    @pl.when(core == 0)
    def _():
        for copy in a2a[1]:
            copy.start()

    @pl.when(at_head)
    def _():
        for b, (bit, other) in enumerate(row_pairs):
            @pl.when(bit == 0)
            def _(b=b):
                pl.semaphore_wait(answer.at[N - 1 + b], 1)

            pl.semaphore_signal(word.at[b], inc=1, device_id=(other, d), device_id_type=MESH)
        for b in range(nrow):
            pl.semaphore_wait(word.at[b], 1)
            for j in range(1, N):
                pl.semaphore_signal(word.at[b], inc=1, device_id=(r, lax.rem(d + j, N)), device_id_type=MESH)

    for copy in args:
        copy.wait()
    load.wait()
    first = (r * N + d) * n

    def pick(i, carry):
        base = pl.multiple_of(i * 8, 8)
        rows = []
        for j in range(8):
            local = head_ids[base + j] - first
            owned = jnp.logical_and(local >= 0, local < n)
            row = tab[pl.ds(jnp.clip(local, 0, n - 1), 1), :]
            rows.append(jnp.where(owned, row, jnp.zeros_like(row)))
        part[pl.ds(base, 8), :] = jnp.concatenate(rows, axis=0)
        return carry

    lax.fori_loop(0, Q // 8, pick, 0)

    def remote(src, dst, sems, at, peer):
        return pltpu.make_async_remote_copy(
            src_ref=src, dst_ref=dst, send_sem=sems[0].at[at], recv_sem=sems[1].at[at],
            device_id=peer, device_id_type=MESH,
        )

    def add_rows(h, dst, dst_at, src, src_at, extra, extra_at):
        rows = min(64, h)

        def add(i, carry):
            step = i * rows
            dst[pl.ds(pl.multiple_of(dst_at + step, 8), rows), :] = (
                src[pl.ds(pl.multiple_of(src_at + step, 8), rows), :]
                + extra[pl.ds(pl.multiple_of(extra_at + step, 8), rows), :]
            )
            return carry

        lax.fori_loop(0, h // rows, add, 0)

    @pl.when(d > 0)
    def _():
        for b in range(nrow):
            pl.semaphore_wait(word.at[b], 1)

    row_bits = list(range(nrow))
    orders = [row_bits, row_bits[:1] + row_bits[:0:-1]]
    ex = (ex_send, ex_recv)

    offset = [0, half_q]
    size = half_q
    into = 0
    for k in range(nrow):
        h = size // 2
        copies = []
        for s in range(2):
            bit, other = bit_and_other(r, orders[s][k])
            gone = pl.multiple_of(offset[s] + (1 - bit) * h, 8)
            copy = remote(
                part.at[pl.ds(gone, h), :],
                recv.at[pl.ds(s * half_q + into, h), :],
                ex, (s, k), (other, d),
            )
            copy.start()
            copies.append(copy)
            offset[s] = pl.multiple_of(offset[s] + bit * h, 8)
        if k == 0:
            def narrow(i, carry):
                at = pl.multiple_of(i * 128, 128)
                low[pl.ds(at, 128), :] = tab[pl.ds(at, 128), :].astype(jnp.bfloat16)
                return carry

            lax.fori_loop(0, n // 128, narrow, 0)
        if k == min(1, nrow - 1):
            idx = thr_idx[...]

            def choose(t, acc):
                return jnp.where(idx == t, thr[t], acc)

            lev[...] = lax.fori_loop(0, thr.shape[0], choose, jnp.zeros(idx.shape, jnp.float32))
        for s in range(2):
            copies[s].wait()
            if k < nrow - 1:
                add_rows(h, part, offset[s], part, offset[s], recv, s * half_q + into)
            else:
                add_rows(h, zsum, (2 * s + core) * h, part, offset[s], recv, s * half_q + into)
        into += h
        size = h

    partner = (r + 1 - 2 * core, d)
    skip = half_q // 2
    core0_at = [pl.multiple_of(offset[s] - core * skip, 8) for s in range(2)]
    pair = (pair_send, pair_recv)
    there_ = [
        remote(zsum.at[pl.ds(2 * s * size, size), :], zsum.at[pl.ds(2 * s * size, size), :], pair, (0, s), partner)
        for s in range(2)
    ]
    back = [
        remote(zout.at[pl.ds(2 * s * size, size), :], full.at[pl.ds(core0_at[s], size), :], pair, (1, s), partner)
        for s in range(2)
    ]
    zx = (z_send, z_recv)

    @pl.when(core == 0)
    def _():
        for copy in there_:
            copy.start()
        for copy in there_:
            copy.wait_send()
        for copy in back:
            copy.wait_recv()

    @pl.when(core == 1)
    def _():
        for copy in there_:
            copy.wait_recv()
        at, count_, into = 0, 4 * size, 0
        for b in range(ndim):
            h = count_ // 2
            bit, other = bit_and_other(d, b)
            gone = pl.multiple_of(at + (1 - bit) * h, 8)
            copy = remote(zsum.at[pl.ds(gone, h), :], zin.at[pl.ds(into, h), :], zx, b, (r, other))
            copy.start()
            at = pl.multiple_of(at + bit * h, 8)
            copy.wait()
            add_rows(h, zsum, at, zsum, at, zin, into)
            into += h
            count_ = h

        def form(i, carry):
            z = pl.multiple_of(at + i * 8, 8)
            slot = z // size
            s = slot // 2
            c = slot - 2 * s
            q = (1 - s) * core0_at[0] + s * core0_at[1] + c * skip + (z - slot * size)
            rows = [rel[pl.ds(rel_ids[q + j], 1), :] for j in range(8)]
            zout[pl.ds(z, 8), :] = zsum[pl.ds(z, 8), :] * jnp.concatenate(rows, axis=0)
            return carry

        lax.fori_loop(0, count_ // 8, form, 0)
        for b in reversed(range(ndim)):
            bit, other = bit_and_other(d, b)
            here = zout.at[pl.ds(at, count_), :]
            copy = remote(here, here, zx, ndim + b, (r, other))
            copy.start()
            if b == 0:
                for late in a2a[1]:
                    late.start()
            copy.wait()
            at = pl.multiple_of(at - bit * count_, 8)
            count_ = 2 * count_
        for copy in back:
            copy.start()
        for s in range(2):
            rows = min(64, size)

            def take(i, carry, s=s):
                step = i * rows
                full[pl.ds(pl.multiple_of(offset[s] + step, 8), rows), :] = (
                    zout[pl.ds(pl.multiple_of((2 * s + 1) * size + step, 8), rows), :]
                )
                return carry

            lax.fori_loop(0, size // rows, take, 0)
        for copy in back:
            copy.wait_send()

    def count_pair(q0, q1):
        qb[:lanes, :] = full[pl.ds(q0, lanes), :].astype(jnp.bfloat16)
        qb[lanes:, :] = full[pl.ds(q1, lanes), :].astype(jnp.bfloat16)
        i0 = q0 // lanes
        i1 = q1 // lanes
        level = jnp.concatenate([lev[i0], lev[i1]], axis=1)
        rows = 512

        def tile(i, acc):
            at = pl.multiple_of(i * rows, rows)
            score = lax.dot_general(
                low[pl.ds(at, rows), :], qb[...], (((1,), (1,)), ((), ())),
                preferred_element_type=jnp.float32,
            )
            soft = jax.nn.sigmoid(sharpness * (score - level))
            return acc + jnp.sum(soft.reshape(rows // 8, 8, 2 * lanes), axis=0)

        acc = lax.fori_loop(0, n // rows, tile, jnp.zeros((8, 2 * lanes), jnp.float32))
        share = jnp.sum(acc, axis=0, keepdims=True) * (1.0 / total_ents)
        frac[i0] = share[:, :lanes]
        frac[i1] = share[:, lanes:]

    def count(starts_, rows):
        def body(i, carry):
            count_pair(pl.multiple_of(starts_[0] + i * lanes, lanes), pl.multiple_of(starts_[1] + i * lanes, lanes))
            return carry

        lax.fori_loop(0, rows // lanes, body, 0)

    pending = None
    counted = False
    if size >= lanes:
        pending = (list(offset), size)
        counted = True
    for k in reversed(range(nrow)):
        copies = []
        there = []
        for s in range(2):
            bit, other = bit_and_other(r, orders[s][k])
            here = full.at[pl.ds(offset[s], size), :]
            copy = remote(here, here, ex, (s, nrow + k), (other, d))
            copy.start()
            copies.append(copy)
            there.append(pl.multiple_of(offset[s] + (1 - 2 * bit) * size, 8))
            offset[s] = pl.multiple_of(offset[s] - bit * size, 8)
        if pending is not None:
            count(*pending)
            pending = None
        for copy in copies:
            copy.wait()
        size = 2 * size
        if size >= lanes:
            pending = (there, size // 2) if counted else (list(offset), size)
            counted = True
    count(*pending)

    per = frac.shape[0] // R
    fx = (f_send, f_recv)
    handed = remote(frac, fr_pair, fx, 0, partner)
    last = remote(fr_all, fr_all, (last_send, last_recv), 0, partner)

    @pl.when(core == 1)
    def _():
        handed.start()
        handed.wait_send()
        last.wait_recv()

    @pl.when(core == 0)
    def _():
        handed.wait_recv()
        frac[...] = frac[...] + fr_pair[...]
        at, held, into = 0, frac.shape[0], 0
        for b in reversed(range(1, nrow)):
            h = held // 2
            bit, other = bit_and_other(r, b)
            copy = remote(frac.at[pl.ds(at + (1 - bit) * h, h)], fr_in.at[pl.ds(into, h)], fx, b, (other, d))
            copy.start()
            at = at + bit * h
            copy.wait()
            frac[pl.ds(at, h)] = frac[pl.ds(at, h)] + fr_in[pl.ds(into, h)]
            into += h
            held = h
        total = frac[pl.ds(at, held)]
        fr_sum[...] = total
        sends = []
        for k, t in enumerate(dim_peers):
            copy = pltpu.make_async_remote_copy(
                src_ref=fr_sum, dst_ref=fr_dim.at[k],
                send_sem=g_send.at[k], recv_sem=g_recv.at[k],
                device_id=(r, t), device_id_type=MESH,
            )
            copy.start()
            sends.append(copy)
        for k in range(N - 1):
            sends[k].wait()
            total = total + fr_dim[k]
        fr_all[...] = total
        last.start()
        last.wait_send()

    mine = frac_out.shape[1]
    row = fr_all[core * per + d * mine // lanes]
    place = lax.rem(d * mine, lanes) // mine
    out = row[:, :mine]
    for j in range(1, lanes // mine):
        out = jnp.where(place == j, row[:, j * mine:(j + 1) * mine], out)
    frac_out[...] = out
    own.wait()
    for copies in a2a:
        for copy in copies:
            copy.wait()


def place(parts, serving, share, serving_out, share_out, sems):
    rows = serving.shape[0] // parts
    copies = [
        pltpu.make_async_copy(
            serving.at[pl.ds(i * rows, rows), :], serving_out.at[pl.ds(i * rows, rows), :], sems.at[i]
        )
        for i in range(parts)
    ]
    copies.append(pltpu.make_async_copy(share, share_out, sems.at[parts]))
    for copy in copies:
        copy.start()
    for copy in copies:
        copy.wait()


def shards(entity_table, relations, thresholds, head_ids, rel_ids, thr_idx):
    R = lax.axis_size("rows")
    N = lax.axis_size("dim")
    n, width = entity_table.shape
    Q = head_ids.shape[0]
    blocks = Q // lanes
    per = blocks // R
    group = 2 * Q // R
    f32 = jnp.float32
    DMA = pltpu.SemaphoreType.DMA
    vmem = pl.BlockSpec(memory_space=pltpu.VMEM)
    hbm = pl.BlockSpec(memory_space=pltpu.HBM)
    anywhere = pl.BlockSpec(memory_space=pl.ANY)
    mine = Q // (R * N)
    operands = [head_ids, rel_ids, thresholds, thr_idx.reshape(blocks, 1, lanes), relations, entity_table]
    if (width // N) % lanes:
        operands.append(entity_table.reshape(n, N, width // N).transpose(1, 0, 2))
    serving, share = pl.pallas_call(
        functools.partial(kernel, R, N, n * R * N),
        out_shape=(
            pltpu.VMEM((n * N, width // N), f32),
            jax.ShapeDtypeStruct((1, mine), f32),
        ),
        in_specs=[hbm] * len(operands),
        out_specs=(anywhere, vmem),
        scratch_shapes=[
            pltpu.SMEM((Q,), jnp.int32),
            pltpu.SMEM((Q,), jnp.int32),
            pltpu.SMEM(thresholds.shape, f32),
            pltpu.VMEM((blocks, 1, lanes), jnp.int32),
            pltpu.VMEM(relations.shape, f32),
            DMA((5,)),
            pltpu.VMEM((n, width), f32),
            pltpu.VMEM((n, width), jnp.bfloat16),
            pltpu.VMEM((Q, width), f32),
            pltpu.VMEM((Q, width), f32),
            pltpu.VMEM((Q, width), f32),
            pltpu.VMEM((group, width), f32),
            pltpu.VMEM((group, width), f32),
            pltpu.VMEM((group, width), f32),
            pltpu.VMEM((2 * lanes, width), jnp.bfloat16),
            pltpu.VMEM((blocks, 1, lanes), f32),
            pltpu.VMEM((blocks, 1, lanes), f32),
            pltpu.VMEM((blocks, 1, lanes), f32),
            pltpu.VMEM((blocks, 1, lanes), f32),
            pltpu.VMEM((N - 1, 2 * per, 1, lanes), f32),
            pltpu.VMEM((2 * per, 1, lanes), f32),
            pltpu.VMEM((2 * per, 1, lanes), f32),
            DMA, DMA,
            DMA((2, N - 1)), DMA((2, N - 1)),
            DMA((2, 2 * bits_of(R))), DMA((2, 2 * bits_of(R))),
            DMA((2 * bits_of(N),)), DMA((2 * bits_of(N),)),
            DMA((2, 2)), DMA((2, 2)),
            DMA((bits_of(R),)), DMA((bits_of(R),)),
            DMA((N - 1,)), DMA((N - 1,)),
            DMA((1,)), DMA((1,)),
            pltpu.SemaphoreType.REGULAR((N - 1 + bits_of(R),)),
            pltpu.SemaphoreType.REGULAR((bits_of(R),)),
        ],
        compiler_params=pltpu.CompilerParams(
            collective_id=0, has_side_effects=True, vmem_limit_bytes=40 * 2**20
        ),
    )(*[pltpu.with_memory_space_constraint(x, pltpu.HBM) for x in operands])
    parts = 8
    serving, share = pl.pallas_call(
        functools.partial(place, parts),
        out_shape=(
            jax.ShapeDtypeStruct(serving.shape, f32),
            jax.ShapeDtypeStruct(share.shape, f32),
        ),
        in_specs=[vmem] * 2,
        out_specs=(anywhere, anywhere),
        scratch_shapes=[DMA((parts + 1,))],
        compiler_params=pltpu.CompilerParams(vmem_limit_bytes=4 * 2**20),
    )(*[pltpu.with_memory_space_constraint(x, pltpu.VMEM) for x in (serving, share)])
    return serving, share.reshape(mine)


def solution(mesh):
    placed = (P(("rows", "dim"), None), P(), P(), P(), P(), P())
    return jax.shard_map(
        shards,
        mesh=mesh,
        in_specs=placed,
        out_specs=(P("rows", "dim"), P(("rows", "dim"))),
        check_vma=False,
    )
```

```python
import functools
import jax
import jax.numpy as jnp
from jax import lax
from jax.sharding import PartitionSpec as P
from jax.experimental import pallas as pl
from jax.experimental.pallas import tpu as pltpu

MESH = pl.DeviceIdType.MESH
sharpness = 2.0
lanes = 128
units = 16
entry = 3


def bits_of(size):
    assert size & (size - 1) == 0
    return size.bit_length() - 1


def kernel(
    R, N, total_ents, head_ids_, rel_ids_, thr_, thr_idx_, rel_, table, *others
):
    slabs = others[:-42]
    (
        serving, frac_out,
        head_ids, rel_ids, thr, thr_idx, rel, arg_sem,
        tab, low, part, recv, full, zsum, zin, zout, qb, lev, frac, fr_pair, fr_in, fr_dim, fr_sum, fr_all,
        load_sem, own_sem, a2a_send, a2a_recv, ex_send, ex_recv, z_send, z_recv,
        pair_send, pair_recv, f_send, f_recv, g_send, g_recv, last_send, last_recv, answer, word,
    ) = others[-42:]
    r = lax.axis_index("rows")
    d = lax.axis_index("dim")
    core = lax.rem(r, 2)
    n, width = table.shape
    slab = width // N
    Q = part.shape[0]
    half_q = Q // 2
    nrow = bits_of(R)
    ndim = bits_of(N)

    def slab_rows(t, start, rows):
        if slabs:
            return slabs[0].at[t, pl.ds(start, rows), :]
        return table.at[pl.ds(start, rows), pl.ds(pl.multiple_of(t * slab, slab), slab)]

    def bit_and_other(me, b):
        bit = lax.rem(me // (2 ** b), 2)
        return bit, me + (1 - 2 * bit) * (2 ** b)

    dim_peers = []
    for k in range(1, N):
        t = d
        for b in range(ndim):
            if k // 2 ** b % 2:
                t = t + (bit_and_other(d, b)[1] - d)
        dim_peers.append(t)
    def ahead(j):
        return (r, lax.rem(d + j, N)), d + j < N

    def behind(j):
        return (r, lax.rem(d + N - j, N)), d >= j

    row_pairs = [bit_and_other(r, b) for b in range(nrow)]
    barrier = pltpu.get_barrier_semaphore()
    leaders = d
    for j in range(1, N):
        peer, leads = ahead(j)

        @pl.when(leads)
        def _(peer=peer):
            pl.semaphore_signal(barrier, inc=1, device_id=peer, device_id_type=MESH)

    at_head = d == 0
    for bit, other in row_pairs:
        leaders = leaders + jnp.where(at_head, bit, 0)

        @pl.when(jnp.logical_and(at_head, bit == 0))
        def _(other=other):
            pl.semaphore_signal(barrier, inc=1, device_id=(other, d), device_id_type=MESH)


    @pl.when(leaders > 0)
    def _():
        pl.semaphore_wait(barrier, leaders)

    for j in range(1, N):
        peer, follows = behind(j)

        @pl.when(follows)
        def _(j=j, peer=peer):
            pl.semaphore_signal(answer.at[j - 1], inc=1, device_id=peer, device_id_type=MESH)


    first_rows = n * entry // units

    def slab_copies(piece):
        start, rows = ((0, first_rows), (first_rows, n - first_rows))[piece]
        return [
            pltpu.make_async_remote_copy(
                src_ref=slab_rows(t, start, rows),
                dst_ref=serving.at[pl.ds(pl.multiple_of(d * n + start, 8), rows), :],
                send_sem=a2a_send.at[piece, k],
                recv_sem=a2a_recv.at[piece, k],
                device_id=(r, t),
                device_id_type=MESH,
            )
            for k, t in enumerate(dim_peers if piece else [lax.rem(d + j, N) for j in range(1, N)])
        ]

    a2a = [slab_copies(0), slab_copies(1)]

    for j in range(1, N):
        @pl.when(d >= j)
        def _(j=j):
            a2a[0][N - j - 1].start()

    for b, (bit, other) in enumerate(row_pairs):
        @pl.when(jnp.logical_and(at_head, bit == 1))
        def _(b=b, other=other):
            pl.semaphore_signal(answer.at[N - 1 + b], inc=1, device_id=(other, d), device_id_type=MESH)

    load = pltpu.make_async_copy(table, tab, load_sem)
    load.start()
    own = pltpu.make_async_copy(
        slab_rows(d, 0, n),
        serving.at[pl.ds(pl.multiple_of(d * n, 8), n), :],
        own_sem,
    )
    own.start()
    pairs = [(head_ids_, head_ids), (rel_ids_, rel_ids), (thr_, thr), (thr_idx_, thr_idx), (rel_, rel)]
    args = [pltpu.make_async_copy(src, dst, arg_sem.at[i]) for i, (src, dst) in enumerate(pairs)]
    for copy in args:
        copy.start()

    for j in range(1, N):
        @pl.when(d + j < N)
        def _(j=j):
            pl.semaphore_wait(answer.at[j - 1], 1)
            a2a[0][j - 1].start()

    @pl.when(core == 0)
    def _():
        for copy in a2a[1]:
            copy.start()

    @pl.when(at_head)
    def _():
        for b, (bit, other) in enumerate(row_pairs):
            @pl.when(bit == 0)
            def _(b=b):
                pl.semaphore_wait(answer.at[N - 1 + b], 1)

            pl.semaphore_signal(word.at[b], inc=1, device_id=(other, d), device_id_type=MESH)
        for b in range(nrow):
            pl.semaphore_wait(word.at[b], 1)
            for j in range(1, N):
                pl.semaphore_signal(word.at[b], inc=1, device_id=(r, lax.rem(d + j, N)), device_id_type=MESH)

    for copy in args:
        copy.wait()
    load.wait()
    first = (r * N + d) * n

    def pick(i, carry):
        base = pl.multiple_of(i * 8, 8)
        rows = []
        for j in range(8):
            local = head_ids[base + j] - first
            owned = jnp.logical_and(local >= 0, local < n)
            row = tab[pl.ds(jnp.clip(local, 0, n - 1), 1), :]
            rows.append(jnp.where(owned, row, jnp.zeros_like(row)))
        part[pl.ds(base, 8), :] = jnp.concatenate(rows, axis=0)
        return carry

    lax.fori_loop(0, Q // 8, pick, 0)

    def remote(src, dst, sems, at, peer):
        return pltpu.make_async_remote_copy(
            src_ref=src, dst_ref=dst, send_sem=sems[0].at[at], recv_sem=sems[1].at[at],
            device_id=peer, device_id_type=MESH,
        )

    def add_rows(h, dst, dst_at, src, src_at, extra, extra_at):
        rows = min(64, h)

        def add(i, carry):
            step = i * rows
            dst[pl.ds(pl.multiple_of(dst_at + step, 8), rows), :] = (
                src[pl.ds(pl.multiple_of(src_at + step, 8), rows), :]
                + extra[pl.ds(pl.multiple_of(extra_at + step, 8), rows), :]
            )
            return carry

        lax.fori_loop(0, h // rows, add, 0)

    @pl.when(d > 0)
    def _():
        for b in range(nrow):
            pl.semaphore_wait(word.at[b], 1)

    row_bits = list(range(nrow))
    orders = [row_bits, row_bits[:1] + row_bits[:0:-1]]
    ex = (ex_send, ex_recv)

    offset = [0, half_q]
    size = half_q
    into = 0
    for k in range(nrow):
        h = size // 2
        copies = []
        for s in range(2):
            bit, other = bit_and_other(r, orders[s][k])
            gone = pl.multiple_of(offset[s] + (1 - bit) * h, 8)
            copy = remote(
                part.at[pl.ds(gone, h), :],
                recv.at[pl.ds(s * half_q + into, h), :],
                ex, (s, k), (other, d),
            )
            copy.start()
            copies.append(copy)
            offset[s] = pl.multiple_of(offset[s] + bit * h, 8)
        if k == 0:
            def narrow(i, carry):
                at = pl.multiple_of(i * 128, 128)
                low[pl.ds(at, 128), :] = tab[pl.ds(at, 128), :].astype(jnp.bfloat16)
                return carry

            lax.fori_loop(0, n // 128, narrow, 0)
        if k == min(1, nrow - 1):
            idx = thr_idx[...]

            def choose(t, acc):
                return jnp.where(idx == t, thr[t], acc)

            lev[...] = lax.fori_loop(0, thr.shape[0], choose, jnp.zeros(idx.shape, jnp.float32))
        for s in range(2):
            copies[s].wait()
            if k < nrow - 1:
                add_rows(h, part, offset[s], part, offset[s], recv, s * half_q + into)
            else:
                add_rows(h, zsum, (2 * s + core) * h, part, offset[s], recv, s * half_q + into)
        into += h
        size = h

    partner = (r + 1 - 2 * core, d)
    skip = half_q // 2
    core0_at = [pl.multiple_of(offset[s] - core * skip, 8) for s in range(2)]
    pair = (pair_send, pair_recv)
    there_ = [
        remote(zsum.at[pl.ds(2 * s * size, size), :], zsum.at[pl.ds(2 * s * size, size), :], pair, (0, s), partner)
        for s in range(2)
    ]
    back = [
        remote(zout.at[pl.ds(2 * s * size, size), :], full.at[pl.ds(core0_at[s], size), :], pair, (1, s), partner)
        for s in range(2)
    ]
    zx = (z_send, z_recv)

    @pl.when(core == 0)
    def _():
        for copy in there_:
            copy.start()
        for copy in there_:
            copy.wait_send()
        for copy in back:
            copy.wait_recv()

    @pl.when(core == 1)
    def _():
        for copy in there_:
            copy.wait_recv()
        at, count_, into = 0, 4 * size, 0
        for b in range(ndim):
            h = count_ // 2
            bit, other = bit_and_other(d, b)
            gone = pl.multiple_of(at + (1 - bit) * h, 8)
            copy = remote(zsum.at[pl.ds(gone, h), :], zin.at[pl.ds(into, h), :], zx, b, (r, other))
            copy.start()
            at = pl.multiple_of(at + bit * h, 8)
            copy.wait()
            add_rows(h, zsum, at, zsum, at, zin, into)
            into += h
            count_ = h

        def form(i, carry):
            z = pl.multiple_of(at + i * 8, 8)
            slot = z // size
            s = slot // 2
            c = slot - 2 * s
            q = (1 - s) * core0_at[0] + s * core0_at[1] + c * skip + (z - slot * size)
            rows = [rel[pl.ds(rel_ids[q + j], 1), :] for j in range(8)]
            zout[pl.ds(z, 8), :] = zsum[pl.ds(z, 8), :] * jnp.concatenate(rows, axis=0)
            return carry

        lax.fori_loop(0, count_ // 8, form, 0)
        for b in reversed(range(ndim)):
            bit, other = bit_and_other(d, b)
            here = zout.at[pl.ds(at, count_), :]
            copy = remote(here, here, zx, ndim + b, (r, other))
            copy.start()
            if b == 0:
                for late in a2a[1]:
                    late.start()
            copy.wait()
            at = pl.multiple_of(at - bit * count_, 8)
            count_ = 2 * count_
        for copy in back:
            copy.start()
        for s in range(2):
            rows = min(64, size)

            def take(i, carry, s=s):
                step = i * rows
                full[pl.ds(pl.multiple_of(offset[s] + step, 8), rows), :] = (
                    zout[pl.ds(pl.multiple_of((2 * s + 1) * size + step, 8), rows), :]
                )
                return carry

            lax.fori_loop(0, size // rows, take, 0)
        for copy in back:
            copy.wait_send()

    def count_pair(q0, q1):
        qb[:lanes, :] = full[pl.ds(q0, lanes), :].astype(jnp.bfloat16)
        qb[lanes:, :] = full[pl.ds(q1, lanes), :].astype(jnp.bfloat16)
        i0 = q0 // lanes
        i1 = q1 // lanes
        level = jnp.concatenate([lev[i0], lev[i1]], axis=1)
        rows = 512

        def tile(i, acc):
            at = pl.multiple_of(i * rows, rows)
            score = lax.dot_general(
                low[pl.ds(at, rows), :], qb[...], (((1,), (1,)), ((), ())),
                preferred_element_type=jnp.float32,
            )
            soft = jax.nn.sigmoid(sharpness * (score - level))
            return acc + jnp.sum(soft.reshape(rows // 8, 8, 2 * lanes), axis=0)

        acc = lax.fori_loop(0, n // rows, tile, jnp.zeros((8, 2 * lanes), jnp.float32))
        share = jnp.sum(acc, axis=0, keepdims=True) * (1.0 / total_ents)
        frac[i0] = share[:, :lanes]
        frac[i1] = share[:, lanes:]

    def count(starts_, rows):
        def body(i, carry):
            count_pair(pl.multiple_of(starts_[0] + i * lanes, lanes), pl.multiple_of(starts_[1] + i * lanes, lanes))
            return carry

        lax.fori_loop(0, rows // lanes, body, 0)

    pending = None
    counted = False
    if size >= lanes:
        pending = (list(offset), size)
        counted = True
    for k in reversed(range(nrow)):
        copies = []
        there = []
        for s in range(2):
            bit, other = bit_and_other(r, orders[s][k])
            here = full.at[pl.ds(offset[s], size), :]
            copy = remote(here, here, ex, (s, nrow + k), (other, d))
            copy.start()
            copies.append(copy)
            there.append(pl.multiple_of(offset[s] + (1 - 2 * bit) * size, 8))
            offset[s] = pl.multiple_of(offset[s] - bit * size, 8)
        if pending is not None:
            count(*pending)
            pending = None
        for copy in copies:
            copy.wait()
        size = 2 * size
        if size >= lanes:
            pending = (there, size // 2) if counted else (list(offset), size)
            counted = True
    count(*pending)

    per = frac.shape[0] // R
    fx = (f_send, f_recv)
    handed = remote(frac, fr_pair, fx, 0, partner)
    last = remote(fr_all, fr_all, (last_send, last_recv), 0, partner)

    @pl.when(core == 1)
    def _():
        handed.start()
        handed.wait_send()
        last.wait_recv()

    @pl.when(core == 0)
    def _():
        handed.wait_recv()
        frac[...] = frac[...] + fr_pair[...]
        at, held, into = 0, frac.shape[0], 0
        for b in reversed(range(1, nrow)):
            h = held // 2
            bit, other = bit_and_other(r, b)
            copy = remote(frac.at[pl.ds(at + (1 - bit) * h, h)], fr_in.at[pl.ds(into, h)], fx, b, (other, d))
            copy.start()
            at = at + bit * h
            copy.wait()
            frac[pl.ds(at, h)] = frac[pl.ds(at, h)] + fr_in[pl.ds(into, h)]
            into += h
            held = h
        total = frac[pl.ds(at, held)]
        fr_sum[...] = total
        sends = []
        for k, t in enumerate(dim_peers):
            copy = pltpu.make_async_remote_copy(
                src_ref=fr_sum, dst_ref=fr_dim.at[k],
                send_sem=g_send.at[k], recv_sem=g_recv.at[k],
                device_id=(r, t), device_id_type=MESH,
            )
            copy.start()
            sends.append(copy)
        for k in range(N - 1):
            sends[k].wait()
            total = total + fr_dim[k]
        fr_all[...] = total
        last.start()
        last.wait_send()

    mine = frac_out.shape[1]
    row = fr_all[core * per + d * mine // lanes]
    place = lax.rem(d * mine, lanes) // mine
    out = row[:, :mine]
    for j in range(1, lanes // mine):
        out = jnp.where(place == j, row[:, j * mine:(j + 1) * mine], out)
    frac_out[...] = out
    own.wait()
    for copies in a2a:
        for copy in copies:
            copy.wait()


def place(parts, serving, share, serving_out, share_out, sems):
    rows = serving.shape[0] // parts
    copies = [
        pltpu.make_async_copy(
            serving.at[pl.ds(i * rows, rows), :], serving_out.at[pl.ds(i * rows, rows), :], sems.at[i]
        )
        for i in range(parts)
    ]
    copies.insert(0, pltpu.make_async_copy(share, share_out, sems.at[parts]))
    for copy in copies:
        copy.start()
    for copy in copies:
        copy.wait()


def shards(entity_table, relations, thresholds, head_ids, rel_ids, thr_idx):
    R = lax.axis_size("rows")
    N = lax.axis_size("dim")
    n, width = entity_table.shape
    Q = head_ids.shape[0]
    blocks = Q // lanes
    per = blocks // R
    group = 2 * Q // R
    f32 = jnp.float32
    DMA = pltpu.SemaphoreType.DMA
    vmem = pl.BlockSpec(memory_space=pltpu.VMEM)
    hbm = pl.BlockSpec(memory_space=pltpu.HBM)
    anywhere = pl.BlockSpec(memory_space=pl.ANY)
    mine = Q // (R * N)
    operands = [head_ids, rel_ids, thresholds, thr_idx.reshape(blocks, 1, lanes), relations, entity_table]
    if (width // N) % lanes:
        operands.append(entity_table.reshape(n, N, width // N).transpose(1, 0, 2))
    serving, share = pl.pallas_call(
        functools.partial(kernel, R, N, n * R * N),
        out_shape=(
            pltpu.VMEM((n * N, width // N), f32),
            jax.ShapeDtypeStruct((1, mine), f32),
        ),
        in_specs=[hbm] * len(operands),
        out_specs=(anywhere, vmem),
        scratch_shapes=[
            pltpu.SMEM((Q,), jnp.int32),
            pltpu.SMEM((Q,), jnp.int32),
            pltpu.SMEM(thresholds.shape, f32),
            pltpu.VMEM((blocks, 1, lanes), jnp.int32),
            pltpu.VMEM(relations.shape, f32),
            DMA((5,)),
            pltpu.VMEM((n, width), f32),
            pltpu.VMEM((n, width), jnp.bfloat16),
            pltpu.VMEM((Q, width), f32),
            pltpu.VMEM((Q, width), f32),
            pltpu.VMEM((Q, width), f32),
            pltpu.VMEM((group, width), f32),
            pltpu.VMEM((group, width), f32),
            pltpu.VMEM((group, width), f32),
            pltpu.VMEM((2 * lanes, width), jnp.bfloat16),
            pltpu.VMEM((blocks, 1, lanes), f32),
            pltpu.VMEM((blocks, 1, lanes), f32),
            pltpu.VMEM((blocks, 1, lanes), f32),
            pltpu.VMEM((blocks, 1, lanes), f32),
            pltpu.VMEM((N - 1, 2 * per, 1, lanes), f32),
            pltpu.VMEM((2 * per, 1, lanes), f32),
            pltpu.VMEM((2 * per, 1, lanes), f32),
            DMA, DMA,
            DMA((2, N - 1)), DMA((2, N - 1)),
            DMA((2, 2 * bits_of(R))), DMA((2, 2 * bits_of(R))),
            DMA((2 * bits_of(N),)), DMA((2 * bits_of(N),)),
            DMA((2, 2)), DMA((2, 2)),
            DMA((bits_of(R),)), DMA((bits_of(R),)),
            DMA((N - 1,)), DMA((N - 1,)),
            DMA((1,)), DMA((1,)),
            pltpu.SemaphoreType.REGULAR((N - 1 + bits_of(R),)),
            pltpu.SemaphoreType.REGULAR((bits_of(R),)),
        ],
        compiler_params=pltpu.CompilerParams(
            collective_id=0, has_side_effects=True, vmem_limit_bytes=40 * 2**20
        ),
    )(*[pltpu.with_memory_space_constraint(x, pltpu.HBM) for x in operands])
    parts = 8
    serving, share = pl.pallas_call(
        functools.partial(place, parts),
        out_shape=(
            jax.ShapeDtypeStruct(serving.shape, f32),
            jax.ShapeDtypeStruct(share.shape, f32),
        ),
        in_specs=[vmem] * 2,
        out_specs=(anywhere, anywhere),
        scratch_shapes=[DMA((parts + 1,))],
        compiler_params=pltpu.CompilerParams(vmem_limit_bytes=4 * 2**20),
    )(*[pltpu.with_memory_space_constraint(x, pltpu.VMEM) for x in (serving, share)])
    return serving, share.reshape(mine)


def solution(mesh):
    placed = (P(("rows", "dim"), None), P(), P(), P(), P(), P())
    return jax.shard_map(
        shards,
        mesh=mesh,
        in_specs=placed,
        out_specs=(P("rows", "dim"), P(("rows", "dim"))),
        check_vma=False,
    )
```
